32 devices in a mesh: net: 4 (over x, core), rep: 8 (over z, y).
Axes of the slice: x: 2, y: 2, z: 4, core: 2. Of those that a mesh axis runs over, the one named last changes fastest.
Arguments:
- latent: bfloat16 [32, 64, 256], P('net', 'rep'), may hold values from -7.2 to 7.2
- hint: bfloat16 [32, 64, 64, 192], P('net', 'rep'), may hold values from -6 to 6
- cond_ids: int32 [32, 1], P('net'), may hold values from 0 to 3; in each aligned block of 8 rows (0 to 7, 8 to 15, ...) at most 4 rows name the same one
- valid: int32 [32], P('net'), may hold values 0 or 1
- cond_scale: float32 [32], P('net'), may hold values from 0.5 to 1.5
- ctl_in: bfloat16 [4, 3, 3, 4, 320], P('net'), may hold values from -1 to 1
- ctl_hint: bfloat16 [4, 192, 320], P('net'), may hold values from -0.4375 to 0.4375
- ctl_zero0: bfloat16 [4, 320, 320], P('net'), may hold values from -0.3125 to 0.3125
- ctl_gain: bfloat16 [4, 320], P('net'), may hold values from 0.099609375 to 1.8984375
- ctl_conv: bfloat16 [4, 3, 3, 320, 320], P('net'), may hold values from -0.109375 to 0.109375
- ctl_zero1: bfloat16 [4, 320, 320], P('net'), may hold values from -0.3125 to 0.3125
- unet_in: bfloat16 [3, 3, 4, 320], replicated, may hold values from -1 to 1
- unet_gain: bfloat16 [320], replicated, may hold values from 0.099609375 to 1.8984375
- unet_conv: bfloat16 [3, 3, 320, 320], replicated, may hold values from -0.109375 to 0.109375
Outputs:
- skip0: bfloat16 [32, 64, 64, 320], P('net', 'rep')
- skip1: bfloat16 [32, 64, 64, 320], P('net', 'rep')
The draws below stay inside these ranges and needn't reach their ends.
Inputs may be any that keep to these rules, and one draw needn't show every extreme that they name: `cond_ids`: in each aligned block of 8 requests (those of one index of net) no id is named by more than 4 requests.
All inputs are finite; a program needn't handle non-finite values. No bound on the sum of `valid` on one device may be relied on, other than what follows from the above.
Results may differ from the reference program's by a relative error of at most 0.008.
Values may be sent and summed in bfloat16 or wider, within the bound.
No kernel may reach another device: no remote copies, remote signals or barrier semaphores. Data moves between devices by JAX's collectives and lax.ppermute only.
A program may use at most 256 MiB of HBM per device.

```python
import math
import jax
import jax.numpy as jnp
import numpy as np
from jax import lax

CH = 320
LCH = 4
GROUPS = 32
HINT = 192
LAT = 64
REQ_GROUP = 8
NETS = 4
PAIR_CAP = 4
REQUESTS = 32
N_NET = 4


def draw_latent(key, part):
    row_place = jnp.arange(LAT, dtype=jnp.float32) / (LAT - 1)
    row_scale = jnp.exp(jnp.log(0.6) + row_place * jnp.log(3.0))
    values = jnp.clip(jax.random.normal(key, (REQUESTS, LAT, LAT * LCH), jnp.float32), -4.0, 4.0)
    return (values * row_scale[None, :, None]).astype(jnp.bfloat16)


def with_ends(entries, stream_key, smallest, top_value):
    longest = entries.shape.index(max(entries.shape))
    spots = []
    for shift in (0, 1):
        where = [jax.random.randint(jax.random.fold_in(stream_key, axis), (), 0, length) for axis, length in enumerate(entries.shape)]
        where[longest] = (where[longest] + shift) % entries.shape[longest]
        spots.append(tuple(where))
    return entries.at[spots[0]].set(smallest).at[spots[1]].set(top_value)


def block_levels(stream_key, shape, pieces, low, high):
    level = 1.0
    for axis_at, parts in pieces:
        heights = jax.random.uniform(jax.random.fold_in(jax.random.fold_in(stream_key, 6), axis_at), (parts,), jnp.float32, low / len(pieces), high / len(pieces))
        level = level * jnp.repeat(jnp.exp(heights), shape[axis_at] // parts).reshape((-1,) + (1,) * (len(shape) - 1 - axis_at))
    return level


def shared_out(rng, own, number, rows, number_of, top, limit, skew):
    order = jax.random.permutation(rng, number_of)
    packed, common = portions_of(number_of, rows * top, limit, skew, True), portions_of(number_of, rows * top, limit, skew, False)
    places = jnp.arange(number_of)

    def named(lengths, rotation):
        used = int((lengths > 0).sum())
        fixed = max(1, used // 4)
        shifted = fixed + (places - fixed + rotation * (used - fixed)) % max(1, number_of - fixed)
        return jnp.zeros((number_of,), jnp.int32).at[order[jnp.where(places < fixed, places, shifted)]].set(jnp.asarray(lengths, jnp.int32))

    lengths = jnp.where(number % 4 == 0, named(packed, number // 4), named(common, number - number // 4 - 1))
    mixed = jax.random.permutation(jax.random.fold_in(own, 3), number_of)
    donor, receiver = mixed[0:number_of // 2 * 2:2], mixed[1:number_of // 2 * 2:2]
    margin = jnp.minimum(lengths[donor] - 1, limit - lengths[receiver]) // 2
    margin = jnp.where((donor == order[0]) | (receiver == order[0]) | (lengths[receiver] == 0), 0, jnp.maximum(margin, 0))
    shifted = jax.random.randint(jax.random.fold_in(own, 4), (number_of // 2,), 0, 1 << 20) % (margin + 1)
    lengths = lengths.at[donor].add(-shifted).at[receiver].add(shifted)
    labels = jnp.searchsorted(jnp.cumsum(lengths), jnp.arange(rows * top), side="right").astype(jnp.int32)
    grid = labels.reshape(top, rows).T
    grid = grid[jax.random.permutation(jax.random.fold_in(own, 1), rows)]
    rotation = jax.random.randint(jax.random.fold_in(own, 2), (rows, 1), 0, top)
    return jnp.take_along_axis(grid, (jnp.arange(top)[None, :] + rotation) % top, axis=1)


def portions_of(amount, total, bound, lean, full):
    weights = [(1 << 20) // math.isqrt(standing ** lean) + 1 for standing in range(1, amount + 1)]
    largest = bound if full else min(bound, max(-(-total // amount), total * weights[0] // sum(weights)))
    least = 1 if total - largest >= amount - 1 else 0
    counts, rest = [largest] + [least] * (amount - 1), total - largest - least * (amount - 1)
    while rest > 0:
        free = [i for i in range(1, amount) if counts[i] < largest] or [i for i in range(1, amount) if counts[i] < bound]
        pool, remaining = sum([weights[i] for i in free]), rest
        for i in free:
            more = min(bound - counts[i], max(1, remaining * weights[i] // pool), rest)
            counts[i] = counts[i] + more
            rest = rest - more
    return np.array(counts)


def gaussian(own_key, dims, scale, most, pieces=(), held_as=jnp.bfloat16):
    values = jax.random.normal(own_key, dims, jnp.float32) * scale
    if len(pieces) > 0:
        values = block_levels(own_key, dims, pieces, -0.22, 0.18) * values
    return jnp.clip(values, min=-most, max=most).astype(held_as)


def setup_inputs(seed: int = 0) -> dict:
    key_list = jax.random.split(jax.random.key(seed), 15)
    latent = draw_latent(jax.random.fold_in(key_list[14], 71), 0)
    hint = gaussian(key_list[1], (REQUESTS, LAT, LAT, HINT), 1.0, 6.0, ((0, 4), (1, 8)))
    cond_ids_keys = jax.random.split(jax.random.fold_in(key_list[2], 1), REQUESTS // REQ_GROUP)
    cond_ids_turns = jax.random.permutation(jax.random.fold_in(key_list[2], 3), REQUESTS // REQ_GROUP)
    cond_ids = jax.vmap(lambda own, number: shared_out(jax.random.fold_in(key_list[2], 2), own, number, REQ_GROUP, N_NET, 1, PAIR_CAP, 2))(cond_ids_keys, cond_ids_turns).reshape((REQUESTS, 1))
    valid = with_ends((jax.random.randint(key_list[3], (REQUESTS,), 0, 8) < 7).astype(jnp.int32), jax.random.fold_in(key_list[3], 1), 0, 1)
    cond_scale = jnp.clip(0.5 + 1.0 * jax.random.uniform(key_list[4], (REQUESTS,), jnp.float32) ** block_levels(key_list[4], (REQUESTS,), ((0, 4),), -0.2, 0.2), 0.5, 1.5)
    ctl_in = gaussian(key_list[5], (NETS, 3, 3, LCH, CH), (9 * LCH) ** -0.5, 1.0, ((0, 4),))
    ctl_hint = gaussian(key_list[6], (NETS, HINT, CH), HINT ** -0.5, 0.4375, ((0, 4),))
    ctl_zero0 = gaussian(key_list[7], (NETS, CH, CH), CH ** -0.5, 0.3125, ((0, 4),))
    ctl_gain = jnp.clip(1.0 + 0.18 * jax.random.normal(key_list[8], (NETS, CH), jnp.float32), 0.099609375, 1.8984375).astype(jnp.bfloat16)
    ctl_conv = gaussian(key_list[9], (NETS, 3, 3, CH, CH), (9 * CH) ** -0.5, 0.109375, ((0, 4),))
    ctl_zero1 = gaussian(key_list[10], (NETS, CH, CH), CH ** -0.5, 0.3125, ((0, 4),))
    unet_in = gaussian(key_list[11], (3, 3, LCH, CH), (9 * LCH) ** -0.5, 1.0)
    unet_gain = jnp.clip(1.0 + 0.18 * jax.random.normal(key_list[12], (CH,), jnp.float32), 0.099609375, 1.8984375).astype(jnp.bfloat16)
    unet_conv = gaussian(key_list[13], (3, 3, CH, CH), (9 * CH) ** -0.5, 0.109375)
    return dict(latent=latent, hint=hint, cond_ids=cond_ids, valid=valid, cond_scale=cond_scale, ctl_in=ctl_in, ctl_hint=ctl_hint, ctl_zero0=ctl_zero0, ctl_gain=ctl_gain, ctl_conv=ctl_conv, ctl_zero1=ctl_zero1, unet_in=unet_in, unet_gain=unet_gain, unet_conv=unet_conv)


epsilon = 1e-05

def conv_rows(padded, weight):
    row_count = padded.shape[-3] - 2
    col_count = padded.shape[-2]
    padding = [(0, 0)] * (padded.ndim - 2) + [(1, 1), (0, 0)]
    padded_cols = jnp.pad(padded, padding)
    result = None
    for shift_y in range(3):
        for shift_x in range(3):
            window = padded_cols[..., shift_y:shift_y + row_count, shift_x:shift_x + col_count, :]
            contribution = jnp.dot(window.reshape(-1, window.shape[-1]), weight[shift_y, shift_x], preferred_element_type=jnp.float32)
            contribution = contribution.reshape(window.shape[:-1] + (weight.shape[-1],))
            result = contribution if result is None else result + contribution
    return result

def project(values, weight):
    flat_out = jnp.dot(values.reshape(-1, values.shape[-1]), weight, preferred_element_type=jnp.float32)
    return flat_out.reshape(values.shape[:-1] + (weight.shape[-1],))

def norm_silu(values, gain):
    floats = values.astype(jnp.float32)
    first_sums = lax.optimization_barrier(jnp.sum(floats, axis=(-3, -2)))
    second_sums = lax.optimization_barrier(jnp.sum(floats * floats, axis=(-3, -2)))
    group_size = values.shape[-1] // GROUPS
    count = values.shape[-3] * values.shape[-2] * group_size
    group_mean = first_sums.reshape(first_sums.shape[:-1] + (GROUPS, group_size)).sum(-1) / count
    group_square = second_sums.reshape(second_sums.shape[:-1] + (GROUPS, group_size)).sum(-1) / count
    inverse = lax.rsqrt(group_square - group_mean * group_mean + epsilon)
    mean_chan = jnp.repeat(group_mean, group_size, axis=-1)
    scale_chan = jnp.repeat(inverse, group_size, axis=-1) * gain.astype(jnp.float32)
    normed = (floats - mean_chan[..., None, None, :]) * scale_chan[..., None, None, :]
    return jax.nn.silu(normed).astype(jnp.bfloat16)

def pad_rows(values):
    return jnp.pad(values, ((1, 1), (0, 0), (0, 0)))

def reference(latent, hint, cond_ids, valid, cond_scale, ctl_in, ctl_hint, ctl_zero0, ctl_gain, ctl_conv, ctl_zero1, unet_in, unet_gain, unet_conv):

    def one_request(request):
        lat_flat, hint_grid, condition, scaling, live = request
        lat_grid = lat_flat.reshape(LAT, LAT, LCH)
        lat_padded = pad_rows(lat_grid)
        first_ctl = (conv_rows(lat_padded, ctl_in[condition]) + project(hint_grid, ctl_hint[condition])).astype(jnp.bfloat16)
        first_res = project(first_ctl, ctl_zero0[condition]).astype(jnp.bfloat16)
        ctl_normed = norm_silu(first_ctl, ctl_gain[condition])
        second_ctl = (first_ctl.astype(jnp.float32) + conv_rows(pad_rows(ctl_normed), ctl_conv[condition])).astype(jnp.bfloat16)
        second_res = project(second_ctl, ctl_zero1[condition]).astype(jnp.bfloat16)
        unet_first = conv_rows(lat_padded, unet_in).astype(jnp.bfloat16)
        unet_normed = norm_silu(unet_first, unet_gain)
        weighting = scaling * live.astype(jnp.float32)
        first_skip = (unet_first.astype(jnp.float32) + weighting * first_res.astype(jnp.float32)).astype(jnp.bfloat16)
        second_skip = (unet_first.astype(jnp.float32) + conv_rows(pad_rows(unet_normed), unet_conv) + weighting * second_res.astype(jnp.float32)).astype(jnp.bfloat16)
        return (first_skip, second_skip)
    skip_first, skip_second = lax.map(one_request, (latent, hint, cond_ids[:, 0], cond_scale, valid))
    return (skip_first, skip_second)
```

```python
import functools

import jax
import jax.numpy as jnp
from jax import lax
from jax.experimental import pallas as pl
from jax.experimental.pallas import tpu as pltpu
from jax.sharding import PartitionSpec as P


LCH = 4
GROUPS = 32
LANES = 128
EPS = 1e-05
CHUNKS = 3


def up_to(value, step):
    return -(-value // step) * step


def cost(flops):
    return pl.CostEstimate(flops=flops, transcendentals=0, bytes_accessed=1 << 20)


def params(mib):
    return pltpu.CompilerParams(
        dimension_semantics=("arbitrary",), vmem_limit_bytes=mib * 1024 * 1024
    )


def main_of(channels):
    return channels // 256 * 256


def slot_of(cond, nets):
    at = lax.axis_index("net")
    return 2 * lax.rem((at >> 1) - (cond >> 1) + nets // 2, nets // 2) + ((at ^ cond) & 1)


def fill_stem(target, hint_weight, in_weight):
    width = hint_weight.shape[0]
    target[0:width, :] = hint_weight.astype(jnp.float32)
    target[width:, :] = jnp.zeros((target.shape[0] - width, target.shape[1]), jnp.float32)
    for dy in range(3):
        for dx in range(3):
            low = width + (3 * dy + dx) * LCH
            target[low : low + LCH, :] = in_weight[dy, dx].astype(jnp.float32)


def compose_kernel(*refs):
    sources, outs = refs[:5], refs[5 : 5 + 2 * CHUNKS]
    conv_ref, hint_ref, in_ref, zero0_ref, zero1_ref, stem, both, whole_half, sems = refs[
        5 + 2 * CHUNKS :
    ]
    copies = [
        pltpu.make_async_copy(src.at[0], dst, sems.at[i])
        for i, (src, dst) in enumerate(
            zip(sources, (conv_ref, hint_ref, in_ref, zero0_ref, zero1_ref))
        )
    ]
    for copy in copies[::-1]:
        copy.start()
    both[...] = jnp.zeros_like(both)
    chans = conv_ref.shape[2]
    part = chans // 2
    main = main_of(chans)
    lanes = up_to(chans, LANES)
    for copy in copies[1:]:
        copy.wait()
    fill_stem(stem, hint_ref[...], in_ref[...])
    both[:, 0:chans] = zero0_ref[...]
    both[:, lanes : lanes + chans] = zero1_ref[...]
    copies[0].wait()
    second_main = both[:, lanes : lanes + main]
    second_tail = both[:, lanes + main : 2 * lanes]
    stem_part = stem.shape[0] // 2
    for order in range(2):
        half = (lax.axis_index("rep") & 1) ^ order
        lhs = stem[pl.ds(half * stem_part, stem_part), :].astype(jnp.bfloat16)
        heads = jnp.dot(lhs, both[...], preferred_element_type=jnp.float32)
        whole_half[0:stem_part, :] = heads.astype(jnp.bfloat16)

        def put(at, width, values):
            whole_half[stem_part:, at : at + width] = values.astype(jnp.bfloat16)

        tails = []
        for dx in range(3):
            lhs = conv_ref[:, dx, pl.ds(half * part, part), :].reshape(3 * part, chans)
            put(dx * main, main, jnp.dot(lhs, second_main, preferred_element_type=jnp.float32))
            tails.append(jnp.dot(lhs, second_tail, preferred_element_type=jnp.float32))
        put(3 * main, LANES, tails[0] + pltpu.roll(tails[1], LANES // 2, 1))
        put(3 * main + LANES, LANES, tails[2])
        low = 0
        for out in outs[CHUNKS * order : CHUNKS * (order + 1)]:
            out[...] = whole_half[low : low + out.shape[0], :]
            low += out.shape[0]


def chunk_rows(rows):
    step = up_to(rows // CHUNKS, 16)
    return [step] * (CHUNKS - 1) + [rows - step * (CHUNKS - 1)]


def compose(ctl_conv, ctl_hint, ctl_in, ctl_zero0, ctl_zero1, depth):
    chans = ctl_conv.shape[3]
    wide = 3 * main_of(chans) + 2 * LANES
    rows = depth // 2 + 3 * (chans // 2)
    shapes = [(size, wide) for size in chunk_rows(rows)] * 2
    sources = (ctl_conv, ctl_hint, ctl_in, ctl_zero0, ctl_zero1)
    return pl.pallas_call(
        compose_kernel,
        in_specs=[pl.BlockSpec(memory_space=pltpu.HBM)] * len(sources),
        out_shape=[jax.ShapeDtypeStruct(shape, jnp.bfloat16) for shape in shapes],
        scratch_shapes=[pltpu.VMEM(array.shape[1:], jnp.bfloat16) for array in sources]
        + [
            pltpu.VMEM((depth, chans), jnp.float32),
            pltpu.VMEM((chans, wide), jnp.bfloat16),
            pltpu.VMEM((rows, wide), jnp.bfloat16),
            pltpu.SemaphoreType.DMA((len(sources),)),
        ],
        compiler_params=pltpu.CompilerParams(vmem_limit_bytes=20 * 1024 * 1024),
        cost_estimate=cost(2 * 1216 * 320 * 1024 * 2),
        name="compose",
    )(*sources)


def arrange_kernel(conv_ref, out_ref):
    chans = conv_ref.shape[2]
    main = main_of(chans)
    tail = chans - main
    row = lax.broadcasted_iota(jnp.int32, (chans, LANES), 0)
    col = lax.broadcasted_iota(jnp.int32, (chans, LANES), 1)
    pick = jnp.where(row == col + main, 1.0, 0.0).astype(jnp.bfloat16)
    for dy in range(3):
        tails = []

        def put(at, values):
            width = values.shape[1]
            out_ref[dy * main : (dy + 1) * main, at : at + width] = values[0:main]
            low = 3 * main + dy * tail
            out_ref[low : low + tail, at : at + width] = values[main:]

        for dx in range(3):
            put(dx * main, conv_ref[dy, dx, :, 0:main])
            tails.append(jnp.dot(conv_ref[dy, dx], pick, preferred_element_type=jnp.float32))
        put(3 * main, (tails[0] + pltpu.roll(tails[1], LANES // 2, 1)).astype(jnp.bfloat16))
        put(3 * main + LANES, tails[2].astype(jnp.bfloat16))
    out_ref[3 * chans :, :] = jnp.zeros(
        (out_ref.shape[0] - 3 * chans, out_ref.shape[1]), jnp.bfloat16
    )


def arrange(unet_conv):
    wide = 3 * main_of(unet_conv.shape[2]) + 2 * LANES
    return pl.pallas_call(
        arrange_kernel,
        out_shape=jax.ShapeDtypeStruct((wide, wide), jnp.bfloat16),
        compiler_params=pltpu.CompilerParams(vmem_limit_bytes=12 * 1024 * 1024),
        cost_estimate=cost(2 * 2880 * 320 * 256),
        name="arrange",
    )(unet_conv)


def stem_kernel(
    cond_ref, lat_ref, hint_ref, top_ref, bot_ref, unet_ref, *rest,
    nets,
):
    stems = rest[: 3 * nets]
    (
        u_ref, h_ref, a_ref, sums_ref, gain_ref,
        weights, grid_in, lone, spread_rows, pick, gains,
    ) = rest[3 * nets :]
    step = pl.program_id(0)
    _, _, double = weights.shape
    half = double // 2
    chans = unet_ref.shape[3]
    _, rows, cols, width = hint_ref.shape
    flat = lat_ref.shape[2]
    bits = LCH.bit_length() - 1

    @pl.when(step == 0)
    def _():
        gains[...] = jnp.zeros_like(gains)
        weights[...] = jnp.zeros_like(weights)
        fill_stem(lone, jnp.zeros((width, chans), jnp.bfloat16), unet_ref[...])
        for n in range(nets):
            weights[n, :, 0:chans] = lone[...].astype(jnp.bfloat16)
        for n in range(nets):
            fill_stem(lone, stems[3 * n + 2][0], stems[3 * n][0])
            weights[n, :, half : half + chans] = lone[...].astype(jnp.bfloat16)
            gains[n : n + 1, 0:chans] = stems[3 * n + 1][...].astype(jnp.float32)
        row = lax.broadcasted_iota(jnp.int32, (flat, LANES), 0)
        col = lax.broadcasted_iota(jnp.int32, (flat, LANES), 1) - width % LANES
        chosen = ((row & (LCH - 1)) == (col & (LCH - 1))) & (col >= 0) & (col < 9 * LCH)
        pick[...] = jnp.where(chosen, 1.0, 0.0).astype(jnp.bfloat16)

    at_x = lax.broadcasted_iota(jnp.int32, (cols, flat), 0)
    of_x = lax.broadcasted_iota(jnp.int32, (cols, flat), 1) >> bits
    lat_rows = (
        [(top_ref, cols + r) for r in range(2)]
        + [(lat_ref, r) for r in range(rows)]
        + [(bot_ref, cols + r) for r in range(2)]
    )
    for i, (ref, r) in enumerate(lat_rows):
        line = ref[0, r : r + 1, :].astype(jnp.float32)
        spread_rows[i * cols : (i + 1) * cols, :] = jnp.where(of_x == at_x, line, 0.0).astype(
            jnp.bfloat16
        )
    cells = jnp.dot(spread_rows[...], pick[...], preferred_element_type=jnp.float32)
    total = (rows + 2) * cols
    size = cells.shape[0]
    tap = (lax.broadcasted_iota(jnp.int32, (1, LANES), 1) - width % LANES) >> bits
    tap_y = (tap >= 3).astype(jnp.int32) + (tap >= 6).astype(jnp.int32)
    tap_x = tap - 3 * tap_y
    place = lax.broadcasted_iota(jnp.int32, (size, 1), 0) & (cols - 1)
    left = jnp.where(place != 0, pltpu.roll(cells, 1, 0), 0.0)
    right = jnp.where(place != cols - 1, pltpu.roll(cells, size - 1, 0), 0.0)
    beside = jnp.where(tap_x == 0, left, jnp.where(tap_x == 1, cells, right))
    patches = jnp.where(
        tap_y == 0,
        beside[0:total],
        jnp.where(tap_y == 1, beside[cols : cols + total], beside[2 * cols :]),
    ).astype(jnp.bfloat16)

    grid_in[0:cols, 0:width] = top_ref[0, 0:cols, 0:width]
    grid_in[cols : total - cols, 0:width] = hint_ref[0].reshape(rows * cols, width)
    grid_in[total - cols : total, 0:width] = bot_ref[0, 0:cols, 0:width]
    grid_in[:, width:] = patches[:, width % LANES :]
    a_ref[0] = grid_in[cols : total - cols, :]
    slot = slot_of(cond_ref[step, 0], nets)
    out = jnp.dot(grid_in[...], weights[slot], preferred_element_type=jnp.float32).astype(
        jnp.bfloat16
    )
    u_ref[0] = out[:, 0:half].reshape(rows + 2, cols, half)
    h_ref[0] = out[:, half:].reshape(rows + 2, cols, half)
    own = out[cols : total - cols].astype(jnp.float32)
    first = jnp.sum(own, axis=0, keepdims=True)
    second = jnp.sum(own * own, axis=0, keepdims=True)
    sums_ref[0] = jnp.concatenate(
        [first[:, 0:half], second[:, 0:half], first[:, half:], second[:, half:]], axis=0
    )
    gain_ref[0] = gains[pl.ds(slot, 1), :]


def whole(array, space=None):
    zeros = (0,) * array.ndim
    if space is not None:
        return pl.BlockSpec(memory_space=space)
    return pl.BlockSpec(array.shape, lambda b: zeros)


def per_request(array):
    rest = (0,) * (array.ndim - 1)
    return pl.BlockSpec((1,) + tuple(array.shape[1:]), lambda b: (b,) + rest)


def stem_call(cond_ids, latent, hint, top, bot, unet_in, stems, depth):
    batch, rows, cols, _ = hint.shape
    nets = len(stems) // 3
    chans = unet_in.shape[3]
    half = up_to(chans, LANES)
    total = (rows + 2) * cols
    flat = latent.shape[2]
    outs = [
        jax.ShapeDtypeStruct((batch, rows + 2, cols, half), jnp.bfloat16),
        jax.ShapeDtypeStruct((batch, rows + 2, cols, half), jnp.bfloat16),
        jax.ShapeDtypeStruct((batch, rows * cols, depth), jnp.bfloat16),
        jax.ShapeDtypeStruct((batch, 4, half), jnp.float32),
        jax.ShapeDtypeStruct((batch, 1, half), jnp.float32),
    ]
    blocked = [latent, hint, top, bot]
    return pl.pallas_call(
        functools.partial(stem_kernel, nets=nets),
        grid=(batch,),
        in_specs=[whole(cond_ids, pltpu.SMEM)]
        + [per_request(array) for array in blocked]
        + [whole(unet_in)]
        + [whole(array) for array in stems],
        out_specs=[per_request(array) for array in outs],
        out_shape=outs,
        scratch_shapes=[
            pltpu.VMEM((nets, depth, 2 * half), jnp.bfloat16),
            pltpu.VMEM((total, depth), jnp.bfloat16),
            pltpu.VMEM((depth, chans), jnp.float32),
            pltpu.VMEM(((rows + 4) * cols, flat), jnp.bfloat16),
            pltpu.VMEM((flat, LANES), jnp.bfloat16),
            pltpu.VMEM((up_to(nets, 8), half), jnp.float32),
        ],
        compiler_params=params(14),
        cost_estimate=cost(2 * batch * total * 256 * 896),
        name="stem",
    )(cond_ids, *blocked, unet_in, *stems)


def group_affine(sums_ref, more_ref, which, gain, count, group, chans, scale_ref, shift_ref):
    lanes = sums_ref.shape[2]
    first = sums_ref[:, 2 * which, :] + more_ref[:, 2 * which, :]
    second = sums_ref[:, 2 * which + 1, :] + more_ref[:, 2 * which + 1, :]
    row = lax.broadcasted_iota(jnp.int32, (lanes, lanes), 0)
    col = lax.broadcasted_iota(jnp.int32, (lanes, lanes), 1)
    row_group = jnp.floor((row.astype(jnp.float32) + 0.5) * (1.0 / group))
    col_group = jnp.floor((col.astype(jnp.float32) + 0.5) * (1.0 / group))
    same = jnp.where((row_group == col_group) & (row < chans), 1.0, 0.0)
    mean = jnp.dot(first, same, precision=lax.Precision.HIGHEST) * (1.0 / count)
    square = jnp.dot(second, same, precision=lax.Precision.HIGHEST) * (1.0 / count)
    scale = lax.rsqrt(square - mean * mean + EPS) * gain
    scale_ref[...] = scale
    shift_ref[...] = -mean * scale


def normed_columns(values, scale, shift, lhs, rows, cols):
    normed = values.astype(jnp.float32) * (0.5 * scale) + 0.5 * shift
    normed = normed + normed * jnp.tanh(normed)
    total = (rows + 2) * cols
    main = main_of(values.shape[1])
    at = lax.axis_index("rep")
    last = lax.axis_size("rep") - 1
    place = lax.broadcasted_iota(jnp.int32, (total, 1), 0)
    keep = ((place >= cols) | (at != 0)) & ((place < total - cols) | (at != last))
    normed = jnp.where(keep, normed, 0.0)
    top = normed[:, 0:main].astype(jnp.bfloat16)
    rest = normed[:, main:]
    inner = rows * cols
    for dy in range(3):
        lhs[:, dy * main : (dy + 1) * main] = top[dy * cols : dy * cols + inner]
    pair = rest[0:inner] + pltpu.roll(rest[cols : cols + inner], LANES // 2, 1)
    lhs[:, 3 * main : 3 * main + LANES] = pair.astype(jnp.bfloat16)
    lhs[:, 3 * main + LANES :] = rest[2 * cols : 2 * cols + inner].astype(jnp.bfloat16)


def spread(product, cols):
    inner = product.shape[0]
    main = product.shape[1] // 4
    place = lax.broadcasted_iota(jnp.int32, (inner, 1), 0) % cols
    left = place != 0
    right = place != cols - 1

    def after(values):
        return jnp.where(left, pltpu.roll(values, 1, 0), 0.0)

    def before(values):
        return jnp.where(right, pltpu.roll(values, inner - 1, 0), 0.0)

    head = (
        after(product[:, 0:main])
        + product[:, main : 2 * main]
        + before(product[:, 2 * main : 3 * main])
    )
    low = product[:, 3 * main : 3 * main + LANES]
    high = product[:, 3 * main + LANES :]
    tail = after(low) + pltpu.roll(low, LANES // 2, 1) + before(high)
    return jnp.concatenate([head, tail], axis=1)


def unet_kernel(
    sums_ref, more_ref, gain_ref, pair_ref, next_ref, weight_ref, out_ref,
    scale, shift, even, odd, *, count, group, chans,
):
    step = pl.program_id(0)
    batch = sums_ref.shape[0]
    _, total_rows, cols, lanes = pair_ref.shape
    rows = total_rows - 2
    inner = rows * cols

    def make(values, b, target):
        values = values.reshape(total_rows * cols, lanes)
        normed_columns(values, scale[pl.ds(b, 1), :], shift[pl.ds(b, 1), :], target, rows, cols)

    def conv(columns, i):
        product = jnp.dot(columns[...], weight_ref[...], preferred_element_type=jnp.float32)
        own = pair_ref[i, 1 : 1 + rows].reshape(inner, lanes).astype(jnp.float32)
        out_ref[i] = spread(product, cols) + own

    @pl.when(step == 0)
    def _():
        gain = jnp.pad(gain_ref[...].astype(jnp.float32), ((0, 0), (0, lanes - chans)))
        group_affine(sums_ref, more_ref, 0, gain, count, group, chans, scale, shift)
        make(pair_ref[0], 0, even)

    make(pair_ref[1], 2 * step + 1, odd)
    conv(even, 0)
    make(next_ref[0], jnp.minimum(2 * step + 2, batch - 1), even)
    conv(odd, 1)


def in_pairs(array):
    rest = (0,) * (array.ndim - 1)
    return pl.BlockSpec((2,) + tuple(array.shape[1:]), lambda b: (b,) + rest)


def next_up(array):
    rest = (0,) * (array.ndim - 1)
    last = array.shape[0] - 1
    return pl.BlockSpec(
        (1,) + tuple(array.shape[1:]), lambda b: (jnp.minimum(2 * b + 2, last),) + rest
    )


def unet_call(sums, more, gain, unet_first, weight, count, group, chans):
    batch, total_rows, cols, lanes = unet_first.shape
    inner = (total_rows - 2) * cols
    depth = weight.shape[0]
    out = jax.ShapeDtypeStruct((batch, inner, lanes), jnp.float32)
    return pl.pallas_call(
        functools.partial(unet_kernel, count=count, group=group, chans=chans),
        grid=(batch // 2,),
        in_specs=[whole(sums), whole(more), whole(gain)]
        + [in_pairs(unet_first), next_up(unet_first), whole(weight)],
        out_specs=in_pairs(out),
        scratch_shapes=[
            pltpu.VMEM((batch, lanes), jnp.float32),
            pltpu.VMEM((batch, lanes), jnp.float32),
            pltpu.VMEM((inner, depth), jnp.bfloat16),
            pltpu.VMEM((inner, depth), jnp.bfloat16),
        ],
        out_shape=out,
        compiler_params=params(24),
        cost_estimate=cost(2 * batch * inner * 1024 * 1024),
        name="unet_conv",
    )(sums, more, gain, unet_first, unet_first, weight)


def control_kernel(
    cond_ref, valid_ref, scale_ref, sums_ref, more_ref, gain_ref, pair_ref, next_ref, a_ref,
    u_ref, base_ref, *rest, nets, count, group, chans,
):
    pieces = rest[: 2 * CHUNKS * nets]
    skip0_ref, skip1_ref, scale, shift, even, odd, weights, heads, sems = rest[
        2 * CHUNKS * nets :
    ]
    step = pl.program_id(0)
    batch = sums_ref.shape[0]
    _, total_rows, cols, lanes = pair_ref.shape
    rows = total_rows - 2
    inner = rows * cols
    main = main_of(chans)
    tail = chans - main
    part = chans // 2
    stem_part = heads.shape[1] // 2

    def segments(n, half):
        yield 0, stem_part, heads, n, half * stem_part
        low, high = half * part, (half + 1) * part
        for dy in range(3):
            first = stem_part + dy * part
            if low < main:
                yield first, min(high, main) - low, weights, n, dy * main + low
            if high > main:
                begin = max(low, main)
                yield (
                    first + begin - low, high - begin, weights, n,
                    3 * main + dy * tail + begin - main,
                )

    def copies(flip):
        made = []
        for n in range(nets):
            for order in range(2):
                bound = 0
                chunks = []
                for piece in pieces[CHUNKS * (2 * n + order) : CHUNKS * (2 * n + order + 1)]:
                    chunks.append((bound, bound + piece.shape[0], piece))
                    bound += piece.shape[0]
                for first, size, target, at, to in segments(n, order ^ flip):
                    for low, high, piece in chunks:
                        start, stop = max(first, low), min(first + size, high)
                        if start < stop:
                            made.append(
                                (
                                    piece.at[
                                        pl.ds(start - low, stop - start),
                                        pl.ds(0, target.shape[2]),
                                    ],
                                    target.at[at, pl.ds(to + start - first, stop - start), :],
                                )
                            )
        return [pltpu.make_async_copy(s, t, sems.at[i]) for i, (s, t) in enumerate(made)]

    def for_side(act):
        for flip in range(2):

            @pl.when((lax.axis_index("rep") & 1) == flip)
            def _():
                for copy in copies(flip):
                    act(copy)

    def make(values, b, target):
        values = values.reshape(total_rows * cols, lanes)
        normed_columns(values, scale[pl.ds(b, 1), :], shift[pl.ds(b, 1), :], target, rows, cols)

    def conv(columns, i):
        b = 2 * step + i
        slot = slot_of(cond_ref[b, 0], nets)
        live = scale_ref[b] * valid_ref[b].astype(jnp.float32)
        heads_out = jnp.dot(a_ref[i], heads[slot], preferred_element_type=jnp.float32)
        own = u_ref[i, 1 : 1 + rows].reshape(inner, lanes).astype(jnp.float32)
        first = own + live * heads_out[:, 0:lanes]
        skip0_ref[i] = first[:, 0:chans].astype(jnp.bfloat16)
        product = jnp.dot(columns[...], weights[slot], preferred_element_type=jnp.float32)
        second = base_ref[i] + live * (spread(product, cols) + heads_out[:, lanes:])
        skip1_ref[i] = second[:, 0:chans].astype(jnp.bfloat16)

    @pl.when(step == 0)
    def _():
        for_side(lambda copy: copy.start())
        for n in range(nets):
            weights[n, 3 * chans :, :] = jnp.zeros(
                (weights.shape[1] - 3 * chans, weights.shape[2]), jnp.bfloat16
            )
        group_affine(sums_ref, more_ref, 1, gain_ref[:, 0, :], count, group, chans, scale, shift)
        make(pair_ref[0], 0, even)
        for_side(lambda copy: copy.wait())

    make(pair_ref[1], 2 * step + 1, odd)
    conv(even, 0)
    make(next_ref[0], jnp.minimum(2 * step + 2, batch - 1), even)
    conv(odd, 1)


def control_call(
    cond_ids, valid, cond_scale, sums, more, gains, control_first, grids, unet_first, base,
    pieces, count, group, chans,
):
    batch, total_rows, cols, lanes = control_first.shape
    inner = (total_rows - 2) * cols
    nets = len(pieces) // (2 * CHUNKS)
    width = pieces[0].shape[1]
    depth = grids.shape[2]
    out = jax.ShapeDtypeStruct((batch, inner, chans), jnp.bfloat16)
    return pl.pallas_call(
        functools.partial(control_kernel, nets=nets, count=count, group=group, chans=chans),
        grid=(batch // 2,),
        in_specs=[whole(array, pltpu.SMEM) for array in (cond_ids, valid, cond_scale)]
        + [whole(sums), whole(more), whole(gains)]
        + [in_pairs(control_first), next_up(control_first)]
        + [in_pairs(array) for array in (grids, unet_first, base)]
        + [whole(array, pl.ANY) for array in pieces],
        out_specs=[in_pairs(out), in_pairs(out)],
        scratch_shapes=[
            pltpu.VMEM((batch, lanes), jnp.float32),
            pltpu.VMEM((batch, lanes), jnp.float32),
            pltpu.VMEM((inner, width), jnp.bfloat16),
            pltpu.VMEM((inner, width), jnp.bfloat16),
            pltpu.VMEM((nets, width, width), jnp.bfloat16),
            pltpu.VMEM((nets, depth, 2 * lanes), jnp.bfloat16),
            pltpu.SemaphoreType.DMA((16 * CHUNKS * nets,)),
        ],
        out_shape=[out, out],
        compiler_params=params(24 + 3 * nets),
        cost_estimate=cost(2 * batch * inner * 1024 * 1280),
        name="control_conv",
    )(
        cond_ids, valid, cond_scale, sums, more, gains, control_first, control_first, grids,
        unet_first, base, *pieces,
    )


def shards(
    latent, hint, cond_ids, valid, cond_scale,
    ctl_in, ctl_hint, ctl_zero0, ctl_gain, ctl_conv, ctl_zero1,
    unet_in, unet_gain, unet_conv,
):
    batch, rows, flat = latent.shape
    cols = flat // LCH
    nets = lax.axis_size("net")
    reps = lax.axis_size("rep")
    chans = unet_gain.shape[0]
    group = chans // GROUPS
    count = rows * reps * cols * group
    depth = up_to(hint.shape[3] + 9 * LCH, 256)

    def moved(arrays, axis, pairs):
        got = []
        for array in arrays:
            got.append(lax.ppermute(array, axis, pairs))
        return got

    def along_net(arrays, offset):
        ring = [(n, (n + 2 * offset) % nets) for n in range(nets)]
        return moved(arrays, "net", ring)

    def across(arrays):
        return moved(arrays, "net", [(n, n ^ 1) for n in range(nets)])

    def beside(arrays, bit=1):
        return moved(arrays, "rep", [(r, r ^ bit) for r in range(reps)])

    small = [ctl_in, ctl_gain, ctl_hint]
    far = [along_net(small, s) for s in range(1, nets // 2)]
    stems = small + across(small)
    for got in far:
        stems += got + across(got)

    def edge(hint_row, lat_rows):
        wide = jnp.pad(hint_row, ((0, 0), (0, 0), (0, flat - hint_row.shape[2])))
        return jnp.pad(jnp.concatenate([wide, lat_rows], axis=1), ((0, 0), (0, 6), (0, 0)))

    down = [(r, r + 1) for r in range(reps - 1)]
    up = [(r + 1, r) for r in range(reps - 1)]
    (top,) = moved([edge(hint[:, rows - 1], latent[:, rows - 2 :])], "rep", down)
    (bot,) = moved([edge(hint[:, 0], latent[:, :2])], "rep", up)

    own = compose(ctl_conv, ctl_hint, ctl_in, ctl_zero0, ctl_zero1, depth)
    away = [along_net(own[:CHUNKS], s) for s in range(1, nets // 2)]
    pieces = list(own) + across(own)
    for got in away:
        full = got + beside(got)
        pieces += full + across(full)

    unet_first, control_first, grids, sums, gains = stem_call(
        cond_ids, latent, hint, top, bot, unet_in, stems, depth
    )
    step = 1
    while 2 * step < reps:
        sums = sums + beside([sums], step)[0]
        step *= 2
    more = beside([sums], step)[0]

    weight = arrange(unet_conv)
    base = unet_call(sums, more, unet_gain[None], unet_first, weight, count, group, chans)
    skip0, skip1 = control_call(
        cond_ids, valid, cond_scale, sums, more, gains, control_first, grids, unet_first, base,
        pieces, count, group, chans,
    )
    shape = (batch, rows, cols, chans)
    return skip0.reshape(shape), skip1.reshape(shape)


def solution(mesh):
    return placed_over(mesh)


def placed_over(mesh):
    return jax.shard_map(
        shards,
        mesh=mesh,
        in_specs=(
            P("net", "rep", None),
            P("net", "rep", None, None),
            P("net", None),
            P("net"),
            P("net"),
            P("net", None, None, None, None),
            P("net", None, None),
            P("net", None, None),
            P("net", None),
            P("net", None, None, None, None),
            P("net", None, None),
            P(),
            P(),
            P(),
        ),
        out_specs=(P("net", "rep", None, None), P("net", "rep", None, None)),
        check_vma=False,
    )
```

```python
import functools

import jax
import jax.numpy as jnp
from jax import lax
from jax.experimental import pallas as pl
from jax.experimental.pallas import tpu as pltpu
from jax.sharding import PartitionSpec as P


LCH = 4
GROUPS = 32
LANES = 128
EPS = 1e-05
CHUNKS = 3


def up_to(value, step):
    return -(-value // step) * step


def cost(flops):
    return pl.CostEstimate(flops=flops, transcendentals=0, bytes_accessed=1 << 20)


def params(mib):
    return pltpu.CompilerParams(
        dimension_semantics=("arbitrary",), vmem_limit_bytes=mib * 1024 * 1024
    )


def main_of(channels):
    return channels // 256 * 256


def slot_of(cond, nets):
    at = lax.axis_index("net")
    return 2 * lax.rem((at >> 1) - (cond >> 1) + nets // 2, nets // 2) + ((at ^ cond) & 1)


def fill_stem(target, hint_weight, in_weight):
    width = hint_weight.shape[0]
    target[0:width, :] = hint_weight.astype(jnp.float32)
    target[width:, :] = jnp.zeros((target.shape[0] - width, target.shape[1]), jnp.float32)
    for dy in range(3):
        for dx in range(3):
            low = width + (3 * dy + dx) * LCH
            target[low : low + LCH, :] = in_weight[dy, dx].astype(jnp.float32)


def compose_kernel(*refs, order):
    sources, outs = refs[:5], refs[5 : 5 + CHUNKS]
    conv_ref, hint_ref, in_ref, zero0_ref, zero1_ref, stem, both, whole_half, sems = refs[
        5 + CHUNKS :
    ]
    copies = [
        pltpu.make_async_copy(src.at[0], dst, sems.at[i])
        for i, (src, dst) in enumerate(
            zip(sources, (conv_ref, hint_ref, in_ref, zero0_ref, zero1_ref))
        )
    ]
    for copy in copies[::-1]:
        copy.start()
    both[...] = jnp.zeros_like(both)
    chans = conv_ref.shape[2]
    part = chans // 2
    main = main_of(chans)
    lanes = up_to(chans, LANES)
    for copy in copies[1:]:
        copy.wait()
    fill_stem(stem, hint_ref[...], in_ref[...])
    both[:, 0:chans] = zero0_ref[...]
    both[:, lanes : lanes + chans] = zero1_ref[...]
    copies[0].wait()
    second_main = both[:, lanes : lanes + main]
    second_tail = both[:, lanes + main : 2 * lanes]
    stem_part = stem.shape[0] // 2
    half = (lax.axis_index("rep") & 1) ^ order
    lhs = stem[pl.ds(half * stem_part, stem_part), :].astype(jnp.bfloat16)
    heads = jnp.dot(lhs, both[...], preferred_element_type=jnp.float32)
    whole_half[0:stem_part, :] = heads.astype(jnp.bfloat16)

    def put(at, width, values):
        whole_half[stem_part:, at : at + width] = values.astype(jnp.bfloat16)

    tails = []
    for dx in range(3):
        lhs = conv_ref[:, dx, pl.ds(half * part, part), :].reshape(3 * part, chans)
        put(dx * main, main, jnp.dot(lhs, second_main, preferred_element_type=jnp.float32))
        tails.append(jnp.dot(lhs, second_tail, preferred_element_type=jnp.float32))
    put(3 * main, LANES, tails[0] + pltpu.roll(tails[1], LANES // 2, 1))
    put(3 * main + LANES, LANES, tails[2])
    low = 0
    for out in outs:
        out[...] = whole_half[low : low + out.shape[0], :]
        low += out.shape[0]


def chunk_rows(rows):
    step = up_to(rows // CHUNKS, 16)
    return [step] * (CHUNKS - 1) + [rows - step * (CHUNKS - 1)]


def compose(order, ctl_conv, ctl_hint, ctl_in, ctl_zero0, ctl_zero1, depth):
    chans = ctl_conv.shape[3]
    wide = 3 * main_of(chans) + 2 * LANES
    rows = depth // 2 + 3 * (chans // 2)
    shapes = [(size, wide) for size in chunk_rows(rows)]
    sources = [far(array) for array in (ctl_conv, ctl_hint, ctl_in, ctl_zero0, ctl_zero1)]
    return pl.pallas_call(
        functools.partial(compose_kernel, order=order),
        in_specs=[pl.BlockSpec(memory_space=pltpu.HBM)] * len(sources),
        out_shape=[jax.ShapeDtypeStruct(shape, jnp.bfloat16) for shape in shapes],
        scratch_shapes=[pltpu.VMEM(array.shape[1:], jnp.bfloat16) for array in sources]
        + [
            pltpu.VMEM((depth, chans), jnp.float32),
            pltpu.VMEM((chans, wide), jnp.bfloat16),
            pltpu.VMEM((rows, wide), jnp.bfloat16),
            pltpu.SemaphoreType.DMA((len(sources),)),
        ],
        compiler_params=pltpu.CompilerParams(vmem_limit_bytes=20 * 1024 * 1024),
        cost_estimate=cost(2 * 608 * 320 * 1024 * 2),
    )(*sources)


def arrange_kernel(conv_ref, out_ref):
    chans = conv_ref.shape[2]
    main = main_of(chans)
    tail = chans - main
    row = lax.broadcasted_iota(jnp.int32, (chans, LANES), 0)
    col = lax.broadcasted_iota(jnp.int32, (chans, LANES), 1)
    pick = jnp.where(row == col + main, 1.0, 0.0).astype(jnp.bfloat16)
    for dy in range(3):
        tails = []

        def put(at, values):
            width = values.shape[1]
            out_ref[dy * main : (dy + 1) * main, at : at + width] = values[0:main]
            low = 3 * main + dy * tail
            out_ref[low : low + tail, at : at + width] = values[main:]

        for dx in range(3):
            put(dx * main, conv_ref[dy, dx, :, 0:main])
            tails.append(jnp.dot(conv_ref[dy, dx], pick, preferred_element_type=jnp.float32))
        put(3 * main, (tails[0] + pltpu.roll(tails[1], LANES // 2, 1)).astype(jnp.bfloat16))
        put(3 * main + LANES, tails[2].astype(jnp.bfloat16))
    out_ref[3 * chans :, :] = jnp.zeros(
        (out_ref.shape[0] - 3 * chans, out_ref.shape[1]), jnp.bfloat16
    )


def arrange(unet_conv):
    wide = 3 * main_of(unet_conv.shape[2]) + 2 * LANES
    return pl.pallas_call(
        arrange_kernel,
        out_shape=jax.ShapeDtypeStruct((wide, wide), jnp.bfloat16),
        compiler_params=pltpu.CompilerParams(vmem_limit_bytes=12 * 1024 * 1024),
        cost_estimate=cost(2 * 2880 * 320 * 256),
        name="arrange",
    )(unet_conv)


def edges_kernel(last_ref, first_ref, lat_ref, next_out, last_out):
    rows = lat_ref.shape[1]
    cols, width = last_ref.shape[2:]
    for out, hint_ref, low in ((next_out, last_ref, rows - 2), (last_out, first_ref, 0)):
        out[...] = jnp.zeros_like(out)
        out[:, 0:cols, 0:width] = hint_ref[:, 0]
        out[:, cols : cols + 2, :] = lat_ref[:, low : low + 2, :]


def edges_call(hint, latent):
    batch, rows, cols, width = hint.shape
    out = jax.ShapeDtypeStruct((batch, cols + 8, latent.shape[2]), jnp.bfloat16)
    return pl.pallas_call(
        edges_kernel,
        grid=(1,),
        in_specs=[
            pl.BlockSpec((batch, 1, cols, width), lambda i: (0, rows - 1, 0, 0)),
            pl.BlockSpec((batch, 1, cols, width), lambda i: (0, 0, 0, 0)),
            pl.BlockSpec(latent.shape, lambda i: (0, 0, 0)),
        ],
        out_specs=[pl.BlockSpec(out.shape, lambda i: (0, 0, 0))] * 2,
        out_shape=[out, out],
        compiler_params=params(8),
        cost_estimate=cost(1 << 20),
        name="edges",
    )(far(hint), far(hint), far(latent))


def stem_kernel(
    cond_ref, lat_ref, hint_ref, top_ref, bot_ref, unet_ref, *rest,
    nets,
):
    stems = rest[: 3 * nets]
    (
        u_ref, h_ref, a_ref, sums_ref, gain_ref,
        weights, grid_in, lone, spread_rows, pick, gains,
    ) = rest[3 * nets :]
    step = pl.program_id(0)
    _, _, double = weights.shape
    half = double // 2
    chans = unet_ref.shape[3]
    _, _, _, width = hint_ref.shape
    flat = lat_ref.shape[2]

    @pl.when(step == 0)
    def _():
        gains[...] = jnp.zeros_like(gains)
        weights[...] = jnp.zeros_like(weights)
        fill_stem(lone, jnp.zeros((width, chans), jnp.bfloat16), unet_ref[...])
        for n in range(nets):
            weights[n, :, 0:chans] = lone[...].astype(jnp.bfloat16)
        for n in range(nets):
            fill_stem(lone, stems[3 * n + 2][0], stems[3 * n][0])
            weights[n, :, half : half + chans] = lone[...].astype(jnp.bfloat16)
            gains[n : n + 1, 0:chans] = stems[3 * n + 1][...].astype(jnp.float32)
        row = lax.broadcasted_iota(jnp.int32, (flat, LANES), 0)
        col = lax.broadcasted_iota(jnp.int32, (flat, LANES), 1) - width % LANES
        chosen = ((row & (LCH - 1)) == (col & (LCH - 1))) & (col >= 0) & (col < 9 * LCH)
        pick[...] = jnp.where(chosen, 1.0, 0.0).astype(jnp.bfloat16)

    for i in range(hint_ref.shape[0]):
        b = hint_ref.shape[0] * step + i
        stem_request(
            i, b, slot_of(cond_ref[b, 0], nets), lat_ref, hint_ref,
            top_ref, bot_ref, u_ref, h_ref, a_ref, sums_ref, gain_ref,
            weights, grid_in.at[i], spread_rows.at[i], pick, gains,
        )


def stem_request(
    i, b, slot, lat_ref, hint_ref, top_ref, bot_ref, u_ref, h_ref, a_ref, sums_ref, gain_ref,
    weights, grid_in, spread_rows, pick, gains,
):
    _, rows, cols, width = hint_ref.shape
    flat = lat_ref.shape[2]
    half = weights.shape[2] // 2
    bits = LCH.bit_length() - 1

    at_x = lax.broadcasted_iota(jnp.int32, (cols, flat), 0)
    of_x = lax.broadcasted_iota(jnp.int32, (cols, flat), 1) >> bits
    lat_rows = (
        [(top_ref, cols + r) for r in range(2)]
        + [(lat_ref, r) for r in range(rows)]
        + [(bot_ref, cols + r) for r in range(2)]
    )
    for j, (ref, r) in enumerate(lat_rows):
        line = ref[i, r : r + 1, :].astype(jnp.float32)
        spread_rows[j * cols : (j + 1) * cols, :] = jnp.where(of_x == at_x, line, 0.0).astype(
            jnp.bfloat16
        )
    cells = jnp.dot(spread_rows[...], pick[...], preferred_element_type=jnp.float32)
    total = (rows + 2) * cols
    size = cells.shape[0]
    tap = (lax.broadcasted_iota(jnp.int32, (1, LANES), 1) - width % LANES) >> bits
    tap_y = (tap >= 3).astype(jnp.int32) + (tap >= 6).astype(jnp.int32)
    tap_x = tap - 3 * tap_y
    place = lax.broadcasted_iota(jnp.int32, (size, 1), 0) & (cols - 1)
    left = jnp.where(place != 0, pltpu.roll(cells, 1, 0), 0.0)
    right = jnp.where(place != cols - 1, pltpu.roll(cells, size - 1, 0), 0.0)
    beside = jnp.where(tap_x == 0, left, jnp.where(tap_x == 1, cells, right))
    patches = jnp.where(
        tap_y == 0,
        beside[0:total],
        jnp.where(tap_y == 1, beside[cols : cols + total], beside[2 * cols :]),
    ).astype(jnp.bfloat16)

    grid_in[0:cols, 0:width] = top_ref[i, 0:cols, 0:width]
    grid_in[cols : total - cols, 0:width] = hint_ref[i].reshape(rows * cols, width)
    grid_in[total - cols : total, 0:width] = bot_ref[i, 0:cols, 0:width]
    grid_in[:, width:] = patches[:, width % LANES :]
    a_ref[b] = grid_in[cols : total - cols, :]
    out = jnp.dot(grid_in[...], weights[slot], preferred_element_type=jnp.float32).astype(
        jnp.bfloat16
    )
    u_ref[b] = out[:, 0:half].reshape(rows + 2, cols, half)
    h_ref[b] = out[:, half:].reshape(rows + 2, cols, half)
    own = out[cols : total - cols].astype(jnp.float32)
    first = jnp.sum(own, axis=0, keepdims=True)
    second = jnp.sum(own * own, axis=0, keepdims=True)
    sums_ref[i] = jnp.concatenate(
        [first[:, 0:half], second[:, 0:half], first[:, half:], second[:, half:]], axis=0
    )
    gain_ref[i] = gains[pl.ds(slot, 1), :]


def far(array):
    return pltpu.with_memory_space_constraint(array, pltpu.HBM)


def whole(array, space=None):
    zeros = (0,) * array.ndim
    if space is not None:
        return pl.BlockSpec(memory_space=space)
    return pl.BlockSpec(array.shape, lambda b: zeros)


def per_request(array, each=1):
    rest = (0,) * (array.ndim - 1)
    return pl.BlockSpec((each,) + tuple(array.shape[1:]), lambda b: (b,) + rest)


def stem_call(cond_ids, latent, hint, top, bot, unet_in, stems, depth):
    batch, rows, cols, _ = hint.shape
    nets = len(stems) // 3
    chans = unet_in.shape[3]
    half = up_to(chans, LANES)
    total = (rows + 2) * cols
    flat = latent.shape[2]
    each = 4 if batch % 4 == 0 else 1
    outs = [
        jax.ShapeDtypeStruct((batch, rows + 2, cols, half), jnp.bfloat16),
        jax.ShapeDtypeStruct((batch, rows + 2, cols, half), jnp.bfloat16),
        jax.ShapeDtypeStruct((batch, rows * cols, depth), jnp.bfloat16),
        jax.ShapeDtypeStruct((batch, 4, half), jnp.float32),
        jax.ShapeDtypeStruct((batch, 1, half), jnp.float32),
    ]
    blocked = [latent, hint, top, bot]
    return pl.pallas_call(
        functools.partial(stem_kernel, nets=nets),
        grid=(batch // each,),
        in_specs=[whole(cond_ids, pltpu.SMEM)]
        + [per_request(array, each) for array in blocked]
        + [whole(unet_in)]
        + [whole(array) for array in stems],
        out_specs=[held()] * 3 + [per_request(array, each) for array in outs[3:]],
        out_shape=outs,
        scratch_shapes=[
            pltpu.VMEM((nets, depth, 2 * half), jnp.bfloat16),
            pltpu.VMEM((each, total, depth), jnp.bfloat16),
            pltpu.VMEM((depth, chans), jnp.float32),
            pltpu.VMEM((each, (rows + 4) * cols, flat), jnp.bfloat16),
            pltpu.VMEM((flat, LANES), jnp.bfloat16),
            pltpu.VMEM((up_to(nets, 8), half), jnp.float32),
        ],
        compiler_params=params(26),
        cost_estimate=cost(2 * batch * total * 256 * 896),
        name="stem",
    )(cond_ids, *blocked, unet_in, *stems)


def group_affine(sums_ref, more_ref, which, gain, count, group, chans, scale_ref, shift_ref):
    lanes = sums_ref.shape[2]
    first = sums_ref[:, 2 * which, :] + more_ref[:, 2 * which, :]
    second = sums_ref[:, 2 * which + 1, :] + more_ref[:, 2 * which + 1, :]
    row = lax.broadcasted_iota(jnp.int32, (lanes, lanes), 0)
    col = lax.broadcasted_iota(jnp.int32, (lanes, lanes), 1)
    row_group = jnp.floor((row.astype(jnp.float32) + 0.5) * (1.0 / group))
    col_group = jnp.floor((col.astype(jnp.float32) + 0.5) * (1.0 / group))
    same = jnp.where((row_group == col_group) & (row < chans), 1.0, 0.0)
    mean = jnp.dot(first, same, precision=lax.Precision.HIGHEST) * (1.0 / count)
    square = jnp.dot(second, same, precision=lax.Precision.HIGHEST) * (1.0 / count)
    scale = lax.rsqrt(square - mean * mean + EPS) * gain
    scale_ref[...] = scale
    shift_ref[...] = -mean * scale


def normed_columns(values, scale, shift, lhs, rows, cols):
    normed = values.astype(jnp.float32) * (0.5 * scale) + 0.5 * shift
    normed = normed + normed * jnp.tanh(normed)
    total = (rows + 2) * cols
    main = main_of(values.shape[1])
    at = lax.axis_index("rep")
    last = lax.axis_size("rep") - 1
    place = lax.broadcasted_iota(jnp.int32, (total, 1), 0)
    keep = ((place >= cols) | (at != 0)) & ((place < total - cols) | (at != last))
    normed = jnp.where(keep, normed, 0.0)
    top = normed[:, 0:main].astype(jnp.bfloat16)
    rest = normed[:, main:]
    inner = rows * cols
    for dy in range(3):
        lhs[:, dy * main : (dy + 1) * main] = top[dy * cols : dy * cols + inner]
    pair = rest[0:inner] + pltpu.roll(rest[cols : cols + inner], LANES // 2, 1)
    lhs[:, 3 * main : 3 * main + LANES] = pair.astype(jnp.bfloat16)
    lhs[:, 3 * main + LANES :] = rest[2 * cols : 2 * cols + inner].astype(jnp.bfloat16)


def spread(columns, weight, product, cols, finish):
    product = jnp.dot(columns, weight, preferred_element_type=jnp.float32)
    inner = product.shape[0]
    main = product.shape[1] // 4
    place = lax.broadcasted_iota(jnp.int32, (inner, 1), 0) % cols
    left = place != 0
    right = place != cols - 1

    def after(values):
        return jnp.where(left, pltpu.roll(values, 1, 0), 0.0)

    def before(values):
        return jnp.where(right, pltpu.roll(values, inner - 1, 0), 0.0)

    head = (
        after(product[:, 0:main])
        + product[:, main : 2 * main]
        + before(product[:, 2 * main : 3 * main])
    )
    low = product[:, 3 * main : 3 * main + LANES]
    high = product[:, 3 * main + LANES :]
    tail = after(low) + pltpu.roll(low, LANES // 2, 1) + before(high)
    finish(0, inner, jnp.concatenate([head, tail], axis=1))


def unet_kernel(
    sums_ref, more_ref, gain_ref, u_ref, weight_ref, out_ref,
    scale, shift, even, odd, product, *, count, group, chans,
):
    step = pl.program_id(0)
    batch = sums_ref.shape[0]
    _, total_rows, cols, lanes = u_ref.shape
    rows = total_rows - 2

    def make(b, target):
        values = u_ref[b].reshape(total_rows * cols, lanes)
        normed_columns(values, scale[pl.ds(b, 1), :], shift[pl.ds(b, 1), :], target, rows, cols)

    def conv(columns, i):
        def finish(at, size, values):
            own = u_ref[2 * step + i, 1 : 1 + rows].reshape(size, lanes).astype(jnp.float32)
            out_ref[2 * step + i, at : at + size] = (values + own).astype(out_ref.dtype)

        spread(columns[...], weight_ref[...], product.at[i], cols, finish)

    @pl.when(step == 0)
    def _():
        gain = jnp.pad(gain_ref[...].astype(jnp.float32), ((0, 0), (0, lanes - chans)))
        group_affine(sums_ref, more_ref, 0, gain, count, group, chans, scale, shift)
        make(0, even)

    make(2 * step + 1, odd)
    conv(even, 0)
    make(jnp.minimum(2 * step + 2, batch - 1), even)
    conv(odd, 1)


def in_pairs(array):
    rest = (0,) * (array.ndim - 1)
    return pl.BlockSpec((2,) + tuple(array.shape[1:]), lambda b: (b,) + rest)


def held():
    return pl.BlockSpec(memory_space=pltpu.VMEM)


def unet_call(sums, more, gain, unet_first, weight, count, group, chans):
    batch, total_rows, cols, lanes = unet_first.shape
    inner = (total_rows - 2) * cols
    depth = weight.shape[0]
    out = jax.ShapeDtypeStruct((batch, inner, lanes), jnp.bfloat16)
    return pl.pallas_call(
        functools.partial(unet_kernel, count=count, group=group, chans=chans),
        grid=(batch // 2,),
        in_specs=[whole(sums), whole(more), whole(gain), held(), held()],
        out_specs=held(),
        scratch_shapes=[
            pltpu.VMEM((batch, lanes), jnp.float32),
            pltpu.VMEM((batch, lanes), jnp.float32),
            pltpu.VMEM((inner, depth), jnp.bfloat16),
            pltpu.VMEM((inner, depth), jnp.bfloat16),
            pltpu.VMEM((2, 8, depth), jnp.float32),
        ],
        out_shape=out,
        compiler_params=params(24),
        cost_estimate=cost(2 * batch * inner * 1024 * 1024),
        name="unet_conv",
    )(sums, more, gain, unet_first, weight)


def control_kernel(
    cond_ref, valid_ref, scale_ref, sums_ref, more_ref, gain_ref, h_ref, a_ref,
    u_ref, base_ref, *rest, nets, count, group, chans,
):
    pieces = rest[: 2 * CHUNKS * nets]
    skip0_ref, skip1_ref, scale, shift, even, odd, product, weights, heads, here, sems = rest[
        2 * CHUNKS * nets :
    ]
    step = pl.program_id(0)
    batch = sums_ref.shape[0]
    _, total_rows, cols, lanes = h_ref.shape
    rows = total_rows - 2
    inner = rows * cols
    main = main_of(chans)
    tail = chans - main
    part = chans // 2
    stem_part = heads.shape[1] // 2

    def segments(n, half):
        yield 0, stem_part, heads, n, half * stem_part
        low, high = half * part, (half + 1) * part
        for dy in range(3):
            first = stem_part + dy * part
            if low < main:
                yield first, min(high, main) - low, weights, n, dy * main + low
            if high > main:
                begin = max(low, main)
                yield (
                    first + begin - low, high - begin, weights, n,
                    3 * main + dy * tail + begin - main,
                )

    def copies(n, flip):
        made = []
        for order in range(2):
            bound = 0
            chunks = []
            for piece in pieces[CHUNKS * (2 * n + order) : CHUNKS * (2 * n + order + 1)]:
                chunks.append((bound, bound + piece.shape[0], piece))
                bound += piece.shape[0]
            for first, size, target, at, to in segments(n, order ^ flip):
                for low, high, piece in chunks:
                    start, stop = max(first, low), min(first + size, high)
                    if start < stop:
                        made.append(
                            (
                                piece.at[
                                    pl.ds(start - low, stop - start), pl.ds(0, target.shape[2])
                                ],
                                target.at[at, pl.ds(to + start - first, stop - start), :],
                            )
                        )
        return [pltpu.make_async_copy(s, t, sems.at[n, i]) for i, (s, t) in enumerate(made)]

    side = lax.axis_index("rep") & 1

    def for_net(n, act):
        for flip in range(2):

            @pl.when(side == flip)
            def _():
                for copy in copies(n, flip):
                    act(copy)

    def need(n):
        @pl.when(here[n] == 0)
        def _():
            for_net(n, lambda copy: copy.wait())
            here[n] = 1

    def soon(n):
        first, second = (slot_of(cond_ref[i, 0], nets) for i in range(2))
        return (first == n) | (second == n)

    def need_slot(slot):
        for n in range(nets):
            pl.when(slot == n)(functools.partial(need, n))

    def make(b, target):
        values = h_ref[b].reshape(total_rows * cols, lanes)
        normed_columns(values, scale[pl.ds(b, 1), :], shift[pl.ds(b, 1), :], target, rows, cols)

    def conv(columns, i):
        b = 2 * step + i
        slot = slot_of(cond_ref[b, 0], nets)
        live = scale_ref[b] * valid_ref[b].astype(jnp.float32)
        heads_out = jnp.dot(a_ref[b], heads[slot], preferred_element_type=jnp.float32)
        own = u_ref[b, 1 : 1 + rows].reshape(inner, lanes).astype(jnp.float32)
        first = own + live * heads_out[:, 0:lanes]
        skip0_ref[i] = first[:, 0:chans].astype(jnp.bfloat16)

        def finish(at, size, values):
            values = values + heads_out[at : at + size, lanes:]
            second = base_ref[b, at : at + size].astype(jnp.float32) + live * values
            skip1_ref[i, at : at + size] = second[:, 0:chans].astype(jnp.bfloat16)

        spread(columns[...], weights[slot], product.at[i], cols, finish)

    @pl.when(step == 0)
    def _():
        for n in range(nets):
            here[n] = 0
            pl.when(soon(n))(functools.partial(for_net, n, lambda copy: copy.start()))
        for n in range(nets):
            weights[n, 3 * chans :, :] = jnp.zeros(
                (weights.shape[1] - 3 * chans, weights.shape[2]), jnp.bfloat16
            )
        group_affine(sums_ref, more_ref, 1, gain_ref[:, 0, :], count, group, chans, scale, shift)
        make(0, even)

    for i in range(2):
        need_slot(slot_of(cond_ref[2 * step + i, 0], nets))

    @pl.when(step == 0)
    def _():
        for n in range(nets):
            pl.when(jnp.logical_not(soon(n)))(
                functools.partial(for_net, n, lambda copy: copy.start())
            )

    make(2 * step + 1, odd)
    conv(even, 0)
    make(jnp.minimum(2 * step + 2, batch - 1), even)
    conv(odd, 1)

    @pl.when(step == pl.num_programs(0) - 1)
    def _():
        for n in range(nets):
            need(n)


def control_call(
    cond_ids, valid, cond_scale, sums, more, gains, control_first, grids, unet_first, base,
    pieces, count, group, chans,
):
    batch, total_rows, cols, lanes = control_first.shape
    inner = (total_rows - 2) * cols
    nets = len(pieces) // (2 * CHUNKS)
    pieces = [far(piece) for piece in pieces]
    width = pieces[0].shape[1]
    depth = grids.shape[2]
    out = jax.ShapeDtypeStruct((batch, inner, chans), jnp.bfloat16)
    return pl.pallas_call(
        functools.partial(control_kernel, nets=nets, count=count, group=group, chans=chans),
        grid=(batch // 2,),
        in_specs=[whole(array, pltpu.SMEM) for array in (cond_ids, valid, cond_scale)]
        + [whole(sums), whole(more), whole(gains)]
        + [held()] * 4
        + [whole(array, pl.ANY) for array in pieces],
        out_specs=[in_pairs(out), in_pairs(out)],
        scratch_shapes=[
            pltpu.VMEM((batch, lanes), jnp.float32),
            pltpu.VMEM((batch, lanes), jnp.float32),
            pltpu.VMEM((inner, width), jnp.bfloat16),
            pltpu.VMEM((inner, width), jnp.bfloat16),
            pltpu.VMEM((2, 8, width), jnp.float32),
            pltpu.VMEM((nets, width, width), jnp.bfloat16),
            pltpu.VMEM((nets, depth, 2 * lanes), jnp.bfloat16),
            pltpu.SMEM((nets,), jnp.int32),
            pltpu.SemaphoreType.DMA((nets, 16 * CHUNKS)),
        ],
        out_shape=[out, out],
        compiler_params=params(24 + 3 * nets),
        cost_estimate=cost(2 * batch * inner * 1024 * 1280),
        name="control_conv",
    )(
        cond_ids, valid, cond_scale, sums, more, gains, control_first, grids,
        unet_first, base, *pieces,
    )


def shards(
    latent, hint, cond_ids, valid, cond_scale,
    ctl_in, ctl_hint, ctl_zero0, ctl_gain, ctl_conv, ctl_zero1,
    unet_in, unet_gain, unet_conv,
):
    batch, rows, flat = latent.shape
    cols = flat // LCH
    nets = lax.axis_size("net")
    reps = lax.axis_size("rep")
    chans = unet_gain.shape[0]
    group = chans // GROUPS
    count = rows * reps * cols * group
    depth = up_to(hint.shape[3] + 9 * LCH, 256)

    def moved(arrays, axis, pairs):
        got = []
        for array in arrays:
            got.append(lax.ppermute(array, axis, pairs))
        return got

    def along_net(arrays, offset):
        ring = [(n, (n + 2 * offset) % nets) for n in range(nets)]
        return moved(arrays, "net", ring)

    def across(arrays):
        return moved(arrays, "net", [(n, n ^ 1) for n in range(nets)])

    def beside(arrays, bit=1):
        return moved(arrays, "rep", [(r, r ^ bit) for r in range(reps)])

    small = [ctl_in, ctl_gain, ctl_hint]
    far = [along_net(small, s) for s in range(1, nets // 2)]
    stems = small + across(small)
    for got in far:
        stems += got + across(got)

    down = [(r, r + 1) for r in range(reps - 1)]
    up = [(r + 1, r) for r in range(reps - 1)]
    to_next, to_last = edges_call(hint, latent)
    (top,) = moved([to_next], "rep", down)
    (bot,) = moved([to_last], "rep", up)

    own = []
    for order in range(2):
        own += compose(order, ctl_conv, ctl_hint, ctl_in, ctl_zero0, ctl_zero1, depth)
    away = [along_net(own[:CHUNKS], s) for s in range(1, nets // 2)]
    pieces = list(own) + across(own)
    for got in away:
        full = got + beside(got)
        pieces += full + across(full)

    unet_first, control_first, grids, sums, gains = stem_call(
        cond_ids, latent, hint, top, bot, unet_in, stems, depth
    )
    step = 1
    while 2 * step < reps:
        sums = sums + beside([sums], step)[0]
        step *= 2
    more = beside([sums], step)[0]

    weight = arrange(unet_conv)
    base = unet_call(sums, more, unet_gain[None], unet_first, weight, count, group, chans)
    skip0, skip1 = control_call(
        cond_ids, valid, cond_scale, sums, more, gains, control_first, grids, unet_first, base,
        pieces, count, group, chans,
    )
    shape = (batch, rows, cols, chans)
    return skip0.reshape(shape), skip1.reshape(shape)


def solution(mesh):
    return placed_over(mesh)


def placed_over(mesh):
    return jax.shard_map(
        shards,
        mesh=mesh,
        in_specs=(
            P("net", "rep", None),
            P("net", "rep", None, None),
            P("net", None),
            P("net"),
            P("net"),
            P("net", None, None, None, None),
            P("net", None, None),
            P("net", None, None),
            P("net", None),
            P("net", None, None, None, None),
            P("net", None, None),
            P(),
            P(),
            P(),
        ),
        out_specs=(P("net", "rep", None, None), P("net", "rep", None, None)),
        check_vma=False,
    )
```

```python
import functools

import jax
import jax.numpy as jnp
from jax import lax
from jax.experimental import pallas as pl
from jax.experimental.pallas import tpu as pltpu
from jax.sharding import PartitionSpec as P


LCH = 4
GROUPS = 32
LANES = 128
EPS = 1e-05
CHUNKS = 2


def up_to(value, step):
    return -(-value // step) * step


def cost(flops):
    return pl.CostEstimate(flops=flops, transcendentals=0, bytes_accessed=1 << 20)


def params(mib):
    return pltpu.CompilerParams(
        dimension_semantics=("arbitrary",), vmem_limit_bytes=mib * 1024 * 1024
    )


def main_of(channels):
    return channels // 256 * 256


def slot_of(cond, nets):
    at = lax.axis_index("net")
    return 2 * lax.rem((at >> 1) - (cond >> 1) + nets // 2, nets // 2) + ((at ^ cond) & 1)


def fill_stem(target, hint_weight, in_weight):
    width = hint_weight.shape[0]
    target[0:width, :] = hint_weight.astype(jnp.float32)
    target[width:, :] = jnp.zeros((target.shape[0] - width, target.shape[1]), jnp.float32)
    for dy in range(3):
        for dx in range(3):
            low = width + (3 * dy + dx) * LCH
            target[low : low + LCH, :] = in_weight[dy, dx].astype(jnp.float32)


def compose_kernel(*refs, order):
    sources, outs = refs[:5], refs[5 : 5 + CHUNKS]
    conv_ref, hint_ref, in_ref, zero0_ref, zero1_ref, stem, both, whole_half, sems = refs[
        5 + CHUNKS :
    ]
    copies = [
        pltpu.make_async_copy(src.at[0], dst, sems.at[i])
        for i, (src, dst) in enumerate(
            zip(sources, (conv_ref, hint_ref, in_ref, zero0_ref, zero1_ref))
        )
    ]
    for copy in copies[::-1]:
        copy.start()
    both[...] = jnp.zeros_like(both)
    chans = conv_ref.shape[2]
    part = chans // 2
    main = main_of(chans)
    lanes = up_to(chans, LANES)
    for copy in copies[1:]:
        copy.wait()
    fill_stem(stem, hint_ref[...], in_ref[...])
    both[:, 0:chans] = zero0_ref[...]
    both[:, lanes : lanes + chans] = zero1_ref[...]
    copies[0].wait()
    second_main = both[:, lanes : lanes + main]
    second_tail = both[:, lanes + main : 2 * lanes]
    stem_part = stem.shape[0] // 2
    half = (lax.axis_index("rep") & 1) ^ order
    lhs = stem[pl.ds(half * stem_part, stem_part), :].astype(jnp.bfloat16)
    heads = jnp.dot(lhs, both[...], preferred_element_type=jnp.float32)
    whole_half[0:stem_part, :] = heads.astype(jnp.bfloat16)

    def put(at, width, values):
        whole_half[stem_part:, at : at + width] = values.astype(jnp.bfloat16)

    tails = []
    for dx in range(3):
        lhs = conv_ref[:, dx, pl.ds(half * part, part), :].reshape(3 * part, chans)
        put(dx * main, main, jnp.dot(lhs, second_main, preferred_element_type=jnp.float32))
        tails.append(jnp.dot(lhs, second_tail, preferred_element_type=jnp.float32))
    put(3 * main, LANES, tails[0] + pltpu.roll(tails[1], LANES // 2, 1))
    put(3 * main + LANES, LANES, tails[2])
    low = 0
    for out in outs:
        out[...] = whole_half[low : low + out.shape[0], :]
        low += out.shape[0]


def chunk_rows(rows):
    step = up_to(rows // CHUNKS, 16)
    return [step] * (CHUNKS - 1) + [rows - step * (CHUNKS - 1)]


def compose(order, ctl_conv, ctl_hint, ctl_in, ctl_zero0, ctl_zero1, depth):
    chans = ctl_conv.shape[3]
    wide = 3 * main_of(chans) + 2 * LANES
    rows = depth // 2 + 3 * (chans // 2)
    shapes = [(size, wide) for size in chunk_rows(rows)]
    sources = [far(array) for array in (ctl_conv, ctl_hint, ctl_in, ctl_zero0, ctl_zero1)]
    return pl.pallas_call(
        functools.partial(compose_kernel, order=order),
        in_specs=[pl.BlockSpec(memory_space=pltpu.HBM)] * len(sources),
        out_shape=[jax.ShapeDtypeStruct(shape, jnp.bfloat16) for shape in shapes],
        scratch_shapes=[pltpu.VMEM(array.shape[1:], jnp.bfloat16) for array in sources]
        + [
            pltpu.VMEM((depth, chans), jnp.float32),
            pltpu.VMEM((chans, wide), jnp.bfloat16),
            pltpu.VMEM((rows, wide), jnp.bfloat16),
            pltpu.SemaphoreType.DMA((len(sources),)),
        ],
        compiler_params=pltpu.CompilerParams(vmem_limit_bytes=20 * 1024 * 1024),
        cost_estimate=cost(2 * 608 * 320 * 1024 * 2),
    )(*sources)


def arrange_kernel(conv_ref, out_ref):
    chans = conv_ref.shape[2]
    main = main_of(chans)
    tail = chans - main
    row = lax.broadcasted_iota(jnp.int32, (chans, LANES), 0)
    col = lax.broadcasted_iota(jnp.int32, (chans, LANES), 1)
    pick = jnp.where(row == col + main, 1.0, 0.0).astype(jnp.bfloat16)
    for dy in range(3):
        tails = []

        def put(at, values):
            width = values.shape[1]
            out_ref[dy * main : (dy + 1) * main, at : at + width] = values[0:main]
            low = 3 * main + dy * tail
            out_ref[low : low + tail, at : at + width] = values[main:]

        for dx in range(3):
            put(dx * main, conv_ref[dy, dx, :, 0:main])
            tails.append(jnp.dot(conv_ref[dy, dx], pick, preferred_element_type=jnp.float32))
        put(3 * main, (tails[0] + pltpu.roll(tails[1], LANES // 2, 1)).astype(jnp.bfloat16))
        put(3 * main + LANES, tails[2].astype(jnp.bfloat16))
    out_ref[3 * chans :, :] = jnp.zeros(
        (out_ref.shape[0] - 3 * chans, out_ref.shape[1]), jnp.bfloat16
    )


def arrange(unet_conv):
    wide = 3 * main_of(unet_conv.shape[2]) + 2 * LANES
    return pl.pallas_call(
        arrange_kernel,
        out_shape=jax.ShapeDtypeStruct((wide, wide), jnp.bfloat16),
        compiler_params=pltpu.CompilerParams(vmem_limit_bytes=12 * 1024 * 1024),
        cost_estimate=cost(2 * 2880 * 320 * 256),
        name="arrange",
    )(unet_conv)


def edges_kernel(last_ref, first_ref, lat_ref, next_out, last_out):
    rows = lat_ref.shape[1]
    cols, width = last_ref.shape[2:]
    for out, hint_ref, low in ((next_out, last_ref, rows - 2), (last_out, first_ref, 0)):
        out[...] = jnp.zeros_like(out)
        out[:, 0:cols, 0:width] = hint_ref[:, 0]
        out[:, cols : cols + 2, :] = lat_ref[:, low : low + 2, :]


def edges_call(hint, latent):
    batch, rows, cols, width = hint.shape
    out = jax.ShapeDtypeStruct((batch, cols + 8, latent.shape[2]), jnp.bfloat16)
    return pl.pallas_call(
        edges_kernel,
        grid=(1,),
        in_specs=[
            pl.BlockSpec((batch, 1, cols, width), lambda i: (0, rows - 1, 0, 0)),
            pl.BlockSpec((batch, 1, cols, width), lambda i: (0, 0, 0, 0)),
            pl.BlockSpec(latent.shape, lambda i: (0, 0, 0)),
        ],
        out_specs=[pl.BlockSpec(out.shape, lambda i: (0, 0, 0))] * 2,
        out_shape=[out, out],
        compiler_params=params(8),
        cost_estimate=cost(1 << 20),
        name="edges",
    )(far(hint), far(hint), far(latent))


def stem_kernel(
    cond_ref, lat_ref, hint_ref, top_ref, bot_ref, unet_ref, *rest,
    nets,
):
    stems = rest[: 3 * nets]
    (
        u_ref, h_ref, a_ref, sums_ref, gain_ref,
        weights, grid_in, lone, spread_rows, pick, gains,
    ) = rest[3 * nets :]
    step = pl.program_id(0)
    _, _, double = weights.shape
    half = double // 2
    chans = unet_ref.shape[3]
    _, _, _, width = hint_ref.shape
    flat = lat_ref.shape[2]

    @pl.when(step == 0)
    def _():
        gains[...] = jnp.zeros_like(gains)
        weights[...] = jnp.zeros_like(weights)
        fill_stem(lone, jnp.zeros((width, chans), jnp.bfloat16), unet_ref[...])
        for n in range(nets):
            weights[n, :, 0:chans] = lone[...].astype(jnp.bfloat16)
        for n in range(nets):
            fill_stem(lone, stems[3 * n + 2][0], stems[3 * n][0])
            weights[n, :, half : half + chans] = lone[...].astype(jnp.bfloat16)
            gains[n : n + 1, 0:chans] = stems[3 * n + 1][...].astype(jnp.float32)
        row = lax.broadcasted_iota(jnp.int32, (flat, LANES), 0)
        col = lax.broadcasted_iota(jnp.int32, (flat, LANES), 1) - width % LANES
        chosen = ((row & (LCH - 1)) == (col & (LCH - 1))) & (col >= 0) & (col < 9 * LCH)
        pick[...] = jnp.where(chosen, 1.0, 0.0).astype(jnp.bfloat16)

    for i in range(hint_ref.shape[0]):
        b = hint_ref.shape[0] * step + i
        stem_request(
            i, b, slot_of(cond_ref[b, 0], nets), lat_ref, hint_ref,
            top_ref, bot_ref, u_ref, h_ref, a_ref, sums_ref, gain_ref,
            weights, grid_in.at[i], spread_rows.at[i], pick, gains,
        )


def stem_request(
    i, b, slot, lat_ref, hint_ref, top_ref, bot_ref, u_ref, h_ref, a_ref, sums_ref, gain_ref,
    weights, grid_in, spread_rows, pick, gains,
):
    _, rows, cols, width = hint_ref.shape
    flat = lat_ref.shape[2]
    half = weights.shape[2] // 2
    bits = LCH.bit_length() - 1

    at_x = lax.broadcasted_iota(jnp.int32, (cols, flat), 0)
    of_x = lax.broadcasted_iota(jnp.int32, (cols, flat), 1) >> bits
    lat_rows = (
        [(top_ref, cols + r) for r in range(2)]
        + [(lat_ref, r) for r in range(rows)]
        + [(bot_ref, cols + r) for r in range(2)]
    )
    for j, (ref, r) in enumerate(lat_rows):
        line = ref[i, r : r + 1, :].astype(jnp.float32)
        spread_rows[j * cols : (j + 1) * cols, :] = jnp.where(of_x == at_x, line, 0.0).astype(
            jnp.bfloat16
        )
    cells = jnp.dot(spread_rows[...], pick[...], preferred_element_type=jnp.float32)
    total = (rows + 2) * cols
    size = cells.shape[0]
    tap = (lax.broadcasted_iota(jnp.int32, (1, LANES), 1) - width % LANES) >> bits
    tap_y = (tap >= 3).astype(jnp.int32) + (tap >= 6).astype(jnp.int32)
    tap_x = tap - 3 * tap_y
    place = lax.broadcasted_iota(jnp.int32, (size, 1), 0) & (cols - 1)
    left = jnp.where(place != 0, pltpu.roll(cells, 1, 0), 0.0)
    right = jnp.where(place != cols - 1, pltpu.roll(cells, size - 1, 0), 0.0)
    beside = jnp.where(tap_x == 0, left, jnp.where(tap_x == 1, cells, right))
    patches = jnp.where(
        tap_y == 0,
        beside[0:total],
        jnp.where(tap_y == 1, beside[cols : cols + total], beside[2 * cols :]),
    ).astype(jnp.bfloat16)

    grid_in[0:cols, 0:width] = top_ref[i, 0:cols, 0:width]
    grid_in[cols : total - cols, 0:width] = hint_ref[i].reshape(rows * cols, width)
    grid_in[total - cols : total, 0:width] = bot_ref[i, 0:cols, 0:width]
    grid_in[:, width:] = patches[:, width % LANES :]
    a_ref[b] = grid_in[cols : total - cols, :]
    out = jnp.dot(grid_in[...], weights[slot], preferred_element_type=jnp.float32).astype(
        jnp.bfloat16
    )
    u_ref[b] = out[:, 0:half].reshape(rows + 2, cols, half)
    h_ref[b] = out[:, half:].reshape(rows + 2, cols, half)
    own = out[cols : total - cols].astype(jnp.float32)
    first = jnp.sum(own, axis=0, keepdims=True)
    second = jnp.sum(own * own, axis=0, keepdims=True)
    sums_ref[i] = jnp.concatenate(
        [first[:, 0:half], second[:, 0:half], first[:, half:], second[:, half:]], axis=0
    )
    gain_ref[i] = gains[pl.ds(slot, 1), :]


def far(array):
    return pltpu.with_memory_space_constraint(array, pltpu.HBM)


def whole(array, space=None):
    zeros = (0,) * array.ndim
    if space is not None:
        return pl.BlockSpec(memory_space=space)
    return pl.BlockSpec(array.shape, lambda b: zeros)


def per_request(array, each=1):
    rest = (0,) * (array.ndim - 1)
    return pl.BlockSpec((each,) + tuple(array.shape[1:]), lambda b: (b,) + rest)


def stem_call(cond_ids, latent, hint, top, bot, unet_in, stems, depth):
    batch, rows, cols, _ = hint.shape
    nets = len(stems) // 3
    chans = unet_in.shape[3]
    half = up_to(chans, LANES)
    total = (rows + 2) * cols
    flat = latent.shape[2]
    each = 4 if batch % 4 == 0 else 1
    outs = [
        jax.ShapeDtypeStruct((batch, rows + 2, cols, half), jnp.bfloat16),
        jax.ShapeDtypeStruct((batch, rows + 2, cols, half), jnp.bfloat16),
        jax.ShapeDtypeStruct((batch, rows * cols, depth), jnp.bfloat16),
        jax.ShapeDtypeStruct((batch, 4, half), jnp.float32),
        jax.ShapeDtypeStruct((batch, 1, half), jnp.float32),
    ]
    blocked = [latent, hint, top, bot]
    return pl.pallas_call(
        functools.partial(stem_kernel, nets=nets),
        grid=(batch // each,),
        in_specs=[whole(cond_ids, pltpu.SMEM)]
        + [per_request(array, each) for array in blocked]
        + [whole(unet_in)]
        + [whole(array) for array in stems],
        out_specs=[held()] * 3 + [per_request(array, each) for array in outs[3:]],
        out_shape=outs,
        scratch_shapes=[
            pltpu.VMEM((nets, depth, 2 * half), jnp.bfloat16),
            pltpu.VMEM((each, total, depth), jnp.bfloat16),
            pltpu.VMEM((depth, chans), jnp.float32),
            pltpu.VMEM((each, (rows + 4) * cols, flat), jnp.bfloat16),
            pltpu.VMEM((flat, LANES), jnp.bfloat16),
            pltpu.VMEM((up_to(nets, 8), half), jnp.float32),
        ],
        compiler_params=params(26),
        cost_estimate=cost(2 * batch * total * 256 * 896),
        name="stem",
    )(cond_ids, *blocked, unet_in, *stems)


def group_affine(sums_ref, more_ref, which, gain, count, group, chans, scale_ref, shift_ref):
    lanes = sums_ref.shape[2]
    first = sums_ref[:, 2 * which, :] + more_ref[:, 2 * which, :]
    second = sums_ref[:, 2 * which + 1, :] + more_ref[:, 2 * which + 1, :]
    row = lax.broadcasted_iota(jnp.int32, (lanes, lanes), 0)
    col = lax.broadcasted_iota(jnp.int32, (lanes, lanes), 1)
    row_group = jnp.floor((row.astype(jnp.float32) + 0.5) * (1.0 / group))
    col_group = jnp.floor((col.astype(jnp.float32) + 0.5) * (1.0 / group))
    same = jnp.where((row_group == col_group) & (row < chans), 1.0, 0.0)
    mean = jnp.dot(first, same, precision=lax.Precision.HIGHEST) * (1.0 / count)
    square = jnp.dot(second, same, precision=lax.Precision.HIGHEST) * (1.0 / count)
    scale = lax.rsqrt(square - mean * mean + EPS) * gain
    scale_ref[...] = scale
    shift_ref[...] = -mean * scale


def normed_columns(values, scale, shift, lhs, rows, cols):
    normed = values.astype(jnp.float32) * (0.5 * scale) + 0.5 * shift
    normed = normed + normed * jnp.tanh(normed)
    total = (rows + 2) * cols
    main = main_of(values.shape[1])
    at = lax.axis_index("rep")
    last = lax.axis_size("rep") - 1
    place = lax.broadcasted_iota(jnp.int32, (total, 1), 0)
    keep = ((place >= cols) | (at != 0)) & ((place < total - cols) | (at != last))
    normed = jnp.where(keep, normed, 0.0)
    top = normed[:, 0:main].astype(jnp.bfloat16)
    rest = normed[:, main:]
    inner = rows * cols
    for dy in range(3):
        lhs[:, dy * main : (dy + 1) * main] = top[dy * cols : dy * cols + inner]
    pair = rest[0:inner] + pltpu.roll(rest[cols : cols + inner], LANES // 2, 1)
    lhs[:, 3 * main : 3 * main + LANES] = pair.astype(jnp.bfloat16)
    lhs[:, 3 * main + LANES :] = rest[2 * cols : 2 * cols + inner].astype(jnp.bfloat16)


def spread(columns, weight, product, cols, finish):
    product = jnp.dot(columns, weight, preferred_element_type=jnp.float32)
    inner = product.shape[0]
    main = product.shape[1] // 4
    place = lax.broadcasted_iota(jnp.int32, (inner, 1), 0) % cols
    left = place != 0
    right = place != cols - 1

    def after(values):
        return jnp.where(left, pltpu.roll(values, 1, 0), 0.0)

    def before(values):
        return jnp.where(right, pltpu.roll(values, inner - 1, 0), 0.0)

    head = (
        after(product[:, 0:main])
        + product[:, main : 2 * main]
        + before(product[:, 2 * main : 3 * main])
    )
    low = product[:, 3 * main : 3 * main + LANES]
    high = product[:, 3 * main + LANES :]
    tail = after(low) + pltpu.roll(low, LANES // 2, 1) + before(high)
    finish(0, inner, jnp.concatenate([head, tail], axis=1))


def unet_kernel(
    sums_ref, more_ref, gain_ref, u_ref, weight_ref, out_ref,
    scale, shift, even, odd, product, *, count, group, chans,
):
    step = pl.program_id(0)
    batch = sums_ref.shape[0]
    _, total_rows, cols, lanes = u_ref.shape
    rows = total_rows - 2

    def make(b, target):
        values = u_ref[b].reshape(total_rows * cols, lanes)
        normed_columns(values, scale[pl.ds(b, 1), :], shift[pl.ds(b, 1), :], target, rows, cols)

    def conv(columns, i):
        def finish(at, size, values):
            own = u_ref[2 * step + i, 1 : 1 + rows].reshape(size, lanes).astype(jnp.float32)
            out_ref[2 * step + i, at : at + size] = (values + own).astype(out_ref.dtype)

        spread(columns[...], weight_ref[...], product.at[i], cols, finish)

    @pl.when(step == 0)
    def _():
        gain = jnp.pad(gain_ref[...].astype(jnp.float32), ((0, 0), (0, lanes - chans)))
        group_affine(sums_ref, more_ref, 0, gain, count, group, chans, scale, shift)
        make(0, even)

    make(2 * step + 1, odd)
    conv(even, 0)
    make(jnp.minimum(2 * step + 2, batch - 1), even)
    conv(odd, 1)


def in_pairs(array):
    rest = (0,) * (array.ndim - 1)
    return pl.BlockSpec((2,) + tuple(array.shape[1:]), lambda b: (b,) + rest)


def held():
    return pl.BlockSpec(memory_space=pltpu.VMEM)


def unet_call(sums, more, gain, unet_first, weight, count, group, chans):
    batch, total_rows, cols, lanes = unet_first.shape
    inner = (total_rows - 2) * cols
    depth = weight.shape[0]
    out = jax.ShapeDtypeStruct((batch, inner, lanes), jnp.bfloat16)
    return pl.pallas_call(
        functools.partial(unet_kernel, count=count, group=group, chans=chans),
        grid=(batch // 2,),
        in_specs=[whole(sums), whole(more), whole(gain), held(), held()],
        out_specs=held(),
        scratch_shapes=[
            pltpu.VMEM((batch, lanes), jnp.float32),
            pltpu.VMEM((batch, lanes), jnp.float32),
            pltpu.VMEM((inner, depth), jnp.bfloat16),
            pltpu.VMEM((inner, depth), jnp.bfloat16),
            pltpu.VMEM((2, 8, depth), jnp.float32),
        ],
        out_shape=out,
        compiler_params=params(24),
        cost_estimate=cost(2 * batch * inner * 1024 * 1024),
        name="unet_conv",
    )(sums, more, gain, unet_first, weight)


def control_kernel(
    cond_ref, valid_ref, scale_ref, sums_ref, more_ref, gain_ref, h_ref, a_ref,
    u_ref, base_ref, *rest, nets, count, group, chans,
):
    pieces = rest[: 2 * CHUNKS * nets]
    skip0_ref, skip1_ref, scale, shift, even, odd, product, weights, heads, here, sems = rest[
        2 * CHUNKS * nets :
    ]
    step = pl.program_id(0)
    batch = sums_ref.shape[0]
    _, total_rows, cols, lanes = h_ref.shape
    rows = total_rows - 2
    inner = rows * cols
    main = main_of(chans)
    tail = chans - main
    part = chans // 2
    stem_part = heads.shape[1] // 2

    def segments(n, half):
        yield 0, stem_part, heads, n, half * stem_part
        low, high = half * part, (half + 1) * part
        for dy in range(3):
            first = stem_part + dy * part
            if low < main:
                yield first, min(high, main) - low, weights, n, dy * main + low
            if high > main:
                begin = max(low, main)
                yield (
                    first + begin - low, high - begin, weights, n,
                    3 * main + dy * tail + begin - main,
                )

    def copies(n, flip):
        made = []
        for order in range(2):
            bound = 0
            chunks = []
            for piece in pieces[CHUNKS * (2 * n + order) : CHUNKS * (2 * n + order + 1)]:
                chunks.append((bound, bound + piece.shape[0], piece))
                bound += piece.shape[0]
            for first, size, target, at, to in segments(n, order ^ flip):
                for low, high, piece in chunks:
                    start, stop = max(first, low), min(first + size, high)
                    if start < stop:
                        made.append(
                            (
                                piece.at[
                                    pl.ds(start - low, stop - start), pl.ds(0, target.shape[2])
                                ],
                                target.at[at, pl.ds(to + start - first, stop - start), :],
                            )
                        )
        return [pltpu.make_async_copy(s, t, sems.at[n, i]) for i, (s, t) in enumerate(made)]

    side = lax.axis_index("rep") & 1

    def for_net(n, act):
        for flip in range(2):

            @pl.when(side == flip)
            def _():
                for copy in copies(n, flip):
                    act(copy)

    def need(n):
        @pl.when(here[n] == 0)
        def _():
            for_net(n, lambda copy: copy.wait())
            here[n] = 1

    def soon(n):
        first, second = (slot_of(cond_ref[i, 0], nets) for i in range(2))
        return (first == n) | (second == n)

    def need_slot(slot):
        for n in range(nets):
            pl.when(slot == n)(functools.partial(need, n))

    def make(b, target):
        values = h_ref[b].reshape(total_rows * cols, lanes)
        normed_columns(values, scale[pl.ds(b, 1), :], shift[pl.ds(b, 1), :], target, rows, cols)

    def conv(columns, i):
        b = 2 * step + i
        slot = slot_of(cond_ref[b, 0], nets)
        live = scale_ref[b] * valid_ref[b].astype(jnp.float32)
        heads_out = jnp.dot(a_ref[b], heads[slot], preferred_element_type=jnp.float32)
        own = u_ref[b, 1 : 1 + rows].reshape(inner, lanes).astype(jnp.float32)
        first = own + live * heads_out[:, 0:lanes]
        skip0_ref[i] = first[:, 0:chans].astype(jnp.bfloat16)

        def finish(at, size, values):
            values = values + heads_out[at : at + size, lanes:]
            second = base_ref[b, at : at + size].astype(jnp.float32) + live * values
            skip1_ref[i, at : at + size] = second[:, 0:chans].astype(jnp.bfloat16)

        spread(columns[...], weights[slot], product.at[i], cols, finish)

    @pl.when(step == 0)
    def _():
        for n in range(nets):
            here[n] = 0
            pl.when(soon(n))(functools.partial(for_net, n, lambda copy: copy.start()))
        for n in range(nets):
            weights[n, 3 * chans :, :] = jnp.zeros(
                (weights.shape[1] - 3 * chans, weights.shape[2]), jnp.bfloat16
            )
        group_affine(sums_ref, more_ref, 1, gain_ref[:, 0, :], count, group, chans, scale, shift)
        make(0, even)

    for i in range(2):
        need_slot(slot_of(cond_ref[2 * step + i, 0], nets))

    @pl.when(step == 0)
    def _():
        for n in range(nets):
            pl.when(jnp.logical_not(soon(n)))(
                functools.partial(for_net, n, lambda copy: copy.start())
            )

    make(2 * step + 1, odd)
    conv(even, 0)
    make(jnp.minimum(2 * step + 2, batch - 1), even)
    conv(odd, 1)

    @pl.when(step == pl.num_programs(0) - 1)
    def _():
        for n in range(nets):
            need(n)


def control_call(
    cond_ids, valid, cond_scale, sums, more, gains, control_first, grids, unet_first, base,
    pieces, count, group, chans,
):
    batch, total_rows, cols, lanes = control_first.shape
    inner = (total_rows - 2) * cols
    nets = len(pieces) // (2 * CHUNKS)
    pieces = [far(piece) for piece in pieces]
    width = pieces[0].shape[1]
    depth = grids.shape[2]
    out = jax.ShapeDtypeStruct((batch, inner, chans), jnp.bfloat16)
    return pl.pallas_call(
        functools.partial(control_kernel, nets=nets, count=count, group=group, chans=chans),
        grid=(batch // 2,),
        in_specs=[whole(array, pltpu.SMEM) for array in (cond_ids, valid, cond_scale)]
        + [whole(sums), whole(more), whole(gains)]
        + [held()] * 4
        + [whole(array, pl.ANY) for array in pieces],
        out_specs=[in_pairs(out), in_pairs(out)],
        scratch_shapes=[
            pltpu.VMEM((batch, lanes), jnp.float32),
            pltpu.VMEM((batch, lanes), jnp.float32),
            pltpu.VMEM((inner, width), jnp.bfloat16),
            pltpu.VMEM((inner, width), jnp.bfloat16),
            pltpu.VMEM((2, 8, width), jnp.float32),
            pltpu.VMEM((nets, width, width), jnp.bfloat16),
            pltpu.VMEM((nets, depth, 2 * lanes), jnp.bfloat16),
            pltpu.SMEM((nets,), jnp.int32),
            pltpu.SemaphoreType.DMA((nets, 16 * CHUNKS)),
        ],
        out_shape=[out, out],
        compiler_params=params(24 + 3 * nets),
        cost_estimate=cost(2 * batch * inner * 1024 * 1280),
        name="control_conv",
    )(
        cond_ids, valid, cond_scale, sums, more, gains, control_first, grids,
        unet_first, base, *pieces,
    )


def shards(
    latent, hint, cond_ids, valid, cond_scale,
    ctl_in, ctl_hint, ctl_zero0, ctl_gain, ctl_conv, ctl_zero1,
    unet_in, unet_gain, unet_conv,
):
    batch, rows, flat = latent.shape
    cols = flat // LCH
    nets = lax.axis_size("net")
    reps = lax.axis_size("rep")
    chans = unet_gain.shape[0]
    group = chans // GROUPS
    count = rows * reps * cols * group
    depth = up_to(hint.shape[3] + 9 * LCH, 256)

    def moved(arrays, axis, pairs):
        got = []
        for array in arrays:
            got.append(lax.ppermute(array, axis, pairs))
        return got

    def along_net(arrays, offset):
        ring = [(n, (n + 2 * offset) % nets) for n in range(nets)]
        return moved(arrays, "net", ring)

    def across(arrays):
        return moved(arrays, "net", [(n, n ^ 1) for n in range(nets)])

    def beside(arrays, bit=1):
        return moved(arrays, "rep", [(r, r ^ bit) for r in range(reps)])

    small = [ctl_in, ctl_gain, ctl_hint]
    far = [along_net(small, s) for s in range(1, nets // 2)]
    stems = small + across(small)
    for got in far:
        stems += got + across(got)

    down = [(r, r + 1) for r in range(reps - 1)]
    up = [(r + 1, r) for r in range(reps - 1)]
    to_next, to_last = edges_call(hint, latent)
    (top,) = moved([to_next], "rep", down)
    (bot,) = moved([to_last], "rep", up)

    own = []
    for order in range(2):
        own += compose(order, ctl_conv, ctl_hint, ctl_in, ctl_zero0, ctl_zero1, depth)
    away = [along_net(own[:CHUNKS], s) for s in range(1, nets // 2)]
    pieces = list(own) + across(own)
    for s, got in enumerate(away):
        late = along_net(own[-1:], s + 1)
        full = got + beside(got[: CHUNKS - 1]) + late
        pieces += full + across(full)

    unet_first, control_first, grids, sums, gains = stem_call(
        cond_ids, latent, hint, top, bot, unet_in, stems, depth
    )
    step = 1
    while 2 * step < reps:
        sums = sums + beside([sums], step)[0]
        step *= 2
    more = beside([sums], step)[0]

    weight = arrange(unet_conv)
    base = unet_call(sums, more, unet_gain[None], unet_first, weight, count, group, chans)
    skip0, skip1 = control_call(
        cond_ids, valid, cond_scale, sums, more, gains, control_first, grids, unet_first, base,
        pieces, count, group, chans,
    )
    shape = (batch, rows, cols, chans)
    return skip0.reshape(shape), skip1.reshape(shape)


def solution(mesh):
    return placed_over(mesh)


def placed_over(mesh):
    return jax.shard_map(
        shards,
        mesh=mesh,
        in_specs=(
            P("net", "rep", None),
            P("net", "rep", None, None),
            P("net", None),
            P("net"),
            P("net"),
            P("net", None, None, None, None),
            P("net", None, None),
            P("net", None, None),
            P("net", None),
            P("net", None, None, None, None),
            P("net", None, None),
            P(),
            P(),
            P(),
        ),
        out_specs=(P("net", "rep", None, None), P("net", "rep", None, None)),
        check_vma=False,
    )
```
